128 devices in a mesh: row: 8 (over y, x_hi), col: 16 (over z, x_lo, core).
Axes of the slice: x: 4 (x_hi: 2, x_lo: 2; x = x_hi * 2 + x_lo), y: 4, z: 4, core: 2. Of those that a mesh axis runs over, the one named last changes fastest.
Arguments:
- noise_points: float32 [32768, 512], P('row'), may hold values from -30 to 30
- data_points: float32 [4096, 512], P('col'), may hold values from -30 to 30
- times: float32 [32768, 8], P(('row', 'col')), may hold values from 0 to 1
- time_shift: float32 [1024], replicated, may hold values from -6 to 6
- weight_in: bfloat16 [512, 1024], replicated, may hold values from -0.25 to 0.25
- weight_out: bfloat16 [1024, 512], replicated, may hold values from -0.1875 to 0.1875
Outputs:
- predicted: bfloat16 [262144, 512], P(('row', 'col'))
- grad_in: float32 [512, 1024], replicated
- grad_out: float32 [1024, 512], replicated
The draws below stay inside these ranges and needn't reach their ends.
All inputs are finite; a program needn't handle non-finite values.
Results may differ from the reference program's by a relative error of at most 0.0057.
Values sent between devices are 32-bit elements; how exact they have to be, the bound alone decides.
A program may use at most 128 MiB of HBM per device.

```python
import math
import jax
import jax.numpy as jnp
from jax import lax

P_SIZE = 512
HID = 1024
NOISE_DEV = 4096
ITERS = 1
TSTEPS = 8
NN = 32768
ND = 4096
N_ROW = 8


def shared_points(key):
    keys = jax.random.split(jax.random.fold_in(key, 7), 2)
    data_base = jnp.clip(jax.random.normal(keys[0], (ND, P_SIZE), jnp.float32), -6.0, 6.0)
    noise_base = jnp.clip(jax.random.normal(keys[1], (NN, P_SIZE), jnp.float32), -6.0, 6.0)
    return (noise_base, data_base)


def draw_noise_points(key, part):
    return shared_points(key)[0]


def draw_data_points(key, part):
    return shared_points(key)[1]


def block_scale(rng, extent, pieces, low, top_value):
    factor_of = 1.0
    for axis_at, shards_of in pieces:
        steps = jax.random.uniform(jax.random.fold_in(jax.random.fold_in(rng, 6), axis_at), (shards_of,), jnp.float32, low / len(pieces), top_value / len(pieces))
        factor_of = factor_of * jnp.repeat(jnp.exp(steps), extent[axis_at] // shards_of).reshape((-1,) + (1,) * (len(extent) - 1 - axis_at))
    return factor_of


def centred(stream_key, shape, deviation, reach, dtype=jnp.bfloat16):
    array = deviation * jax.random.normal(stream_key, shape, jnp.float32)
    return jnp.clip(array, min=-reach, max=reach).astype(dtype)


def setup_inputs(seed: int = 0) -> dict:
    streams_of = jax.random.split(jax.random.key(seed), 7)
    noise_points = draw_noise_points(jax.random.fold_in(streams_of[6], 71), 0)
    data_points = draw_data_points(jax.random.fold_in(streams_of[6], 71), 0)
    times = jnp.clip(1.0 * jax.random.uniform(streams_of[2], (NN, TSTEPS), jnp.float32) ** block_scale(streams_of[2], (NN, TSTEPS), ((0, 128),), -0.2, 0.2), 0.0, 1.0)
    time_shift = centred(streams_of[3], (HID,), 1.0, 6.0, jnp.float32)
    weight_in = centred(streams_of[4], (P_SIZE, HID), P_SIZE ** -0.5, 0.25)
    weight_out = centred(streams_of[5], (HID, P_SIZE), HID ** -0.5, 0.1875)
    return dict(noise_points=noise_points, data_points=data_points, times=times, time_shift=time_shift, weight_in=weight_in, weight_out=weight_out)


ENTROPY = 0.05
HIGHEST_PREC = lax.Precision.HIGHEST

def cost_block(noise_block, data_all):
    noise_sq = lax.optimization_barrier(jnp.sum(noise_block * noise_block, axis=1))
    data_sq = lax.optimization_barrier(jnp.sum(data_all * data_all, axis=1))
    inner = jnp.dot(noise_block, data_all.T, precision=HIGHEST_PREC, preferred_element_type=jnp.float32)
    return (noise_sq[:, None] + data_sq[None, :] - 2.0 * inner) / P_SIZE

def reference(noise_points, data_points, times, time_shift, weight_in, weight_out):
    blocks = noise_points.reshape(N_ROW, NOISE_DEV, P_SIZE)
    potential_g = jnp.zeros((ND,), jnp.float32)
    for sweep in range(ITERS):

        def row_pass(block):
            scores = (potential_g[None, :] - cost_block(block, data_points)) / ENTROPY
            peak = lax.optimization_barrier(jnp.max(scores, axis=1))
            total = lax.optimization_barrier(jnp.sum(jnp.exp(scores - peak[:, None]), axis=1))
            return -ENTROPY * (peak + jnp.log(total) - math.log(float(ND)))
        potential_f = lax.map(row_pass, blocks)

        def col_step(carry, pair):
            block, f_part = pair
            scores = (f_part[:, None] - cost_block(block, data_points)) / ENTROPY
            new_peak = jnp.maximum(carry[0], lax.optimization_barrier(jnp.max(scores, axis=0)))
            total = carry[1] * jnp.exp(carry[0] - new_peak) + lax.optimization_barrier(jnp.sum(jnp.exp(scores - new_peak[None, :]), axis=0))
            return ((new_peak, total), None)
        start = (jnp.full((ND,), -jnp.inf, jnp.float32), jnp.zeros((ND,), jnp.float32))
        (peak_all, total_all), unused = lax.scan(col_step, start, (blocks, potential_f))
        potential_g = -ENTROPY * (peak_all + jnp.log(total_all) - math.log(float(NN)))

    def target_pass(block):
        scores = (potential_g[None, :] - cost_block(block, data_points)) / ENTROPY
        peak = lax.optimization_barrier(jnp.max(scores, axis=1))
        weights = jnp.exp(scores - peak[:, None])
        numer = jnp.dot(weights, data_points, precision=HIGHEST_PREC, preferred_element_type=jnp.float32)
        return numer / lax.optimization_barrier(jnp.sum(weights, axis=1))[:, None]
    target = lax.map(target_pass, blocks).reshape(NN, P_SIZE)
    tvals = times[:, :, None]
    mixed = ((1.0 - tvals) * noise_points[:, None, :] + tvals * target[:, None, :]).reshape(NN * TSTEPS, P_SIZE).astype(jnp.bfloat16)
    velocity = jnp.broadcast_to((target - noise_points)[:, None, :], (NN, TSTEPS, P_SIZE)).reshape(NN * TSTEPS, P_SIZE)
    pre = jnp.dot(mixed, weight_in, preferred_element_type=jnp.float32) + times.reshape(NN * TSTEPS, 1) * time_shift[None, :]
    hidden = jax.nn.silu(pre).astype(jnp.bfloat16)
    output = jnp.dot(hidden, weight_out, preferred_element_type=jnp.float32)
    predicted = output.astype(jnp.bfloat16)
    scale = 1.0 / math.sqrt(float(NN * TSTEPS))
    delta = ((output - velocity) * scale).astype(jnp.bfloat16)
    grad_out = lax.dot_general(hidden, delta, (((0,), (0,)), ((), ())), preferred_element_type=jnp.float32)
    back = lax.dot_general(delta, weight_out, (((1,), (1,)), ((), ())), preferred_element_type=jnp.float32)
    sig = jax.nn.sigmoid(pre)
    delta_pre = (back * sig * (1.0 + pre * (1.0 - sig))).astype(jnp.bfloat16)
    grad_in = lax.dot_general(mixed, delta_pre, (((0,), (0,)), ((), ())), preferred_element_type=jnp.float32)
    return (predicted, grad_in, grad_out)
```

```python
import functools
import math

import jax
import jax.numpy as jnp
from jax import lax
from jax.experimental import pallas as pl
from jax.experimental.pallas import tpu as pltpu
from jax.sharding import PartitionSpec as P

ENTROPY = 0.05
HIGH_PREC = lax.Precision.HIGH
MESH = pl.DeviceIdType.MESH
VMEM_CAP = 60 * 1024 * 1024


class Place:
    def __init__(self):
        row, col = lax.axis_index("row"), lax.axis_index("col")
        self.core = col % 2
        x = (row % 2) * 2 + (col // 2) % 2
        y = row // 2
        z = col // 4
        self.bits = []
        for pos in (x, y, z):
            self.bits.append(((pos + pos // 2) % 2, pos // 2))
        (xa, xb), (ya, yb), (za, zb) = self.bits
        self.groups = ((xa, ya), (yb, za), (zb, xb))
        self.q = tuple(u * 2 + v for u, v in self.groups)
        self.row, self.col = row, col

    def partner(self, group, flip):
        hi, lo = flip // 2, flip % 2
        groups = [list(g) for g in self.groups]
        if hi:
            groups[group][0] = 1 - groups[group][0]
        if lo:
            groups[group][1] = 1 - groups[group][1]
        (xa, ya), (yb, za), (zb, xb) = groups
        x, y, z = ((2 * b + (a + b) % 2) for a, b in ((xa, xb), (ya, yb), (za, zb)))
        return (y * 2 + x // 2, z * 4 + (x % 2) * 2 + self.core)

    def other_core(self):
        return (self.row, self.col + 1 - 2 * self.core)

    def flipped(self, group, flip):
        hi, lo = self.groups[group]
        if flip // 2:
            hi = 1 - hi
        if flip % 2:
            lo = 1 - lo
        return hi * 2 + lo


def meet(place):
    barrier = pltpu.get_barrier_semaphore()
    pl.semaphore_signal(barrier, inc=1, device_id=place.other_core(), device_id_type=MESH)
    for group in range(3):
        for flip in (1, 2, 3):
            pl.semaphore_signal(
                barrier, inc=1, device_id=place.partner(group, flip), device_id_type=MESH
            )
    pl.semaphore_wait(barrier, 10)


def at_groups(turn, first=None, second=None, third=None):
    found = [slice(None)] * 3
    for k, value in enumerate((first, second, third)):
        if value is not None:
            found[(turn + k) % 3] = value
    return tuple(found)


def gather_phases(place, out, pieces, sems, base):
    send, recv = sems
    mine = out.at[place.core]
    started = []

    def copy(src, dst, number, device):
        made = pltpu.make_async_remote_copy(
            src_ref=src, dst_ref=dst, send_sem=send.at[number], recv_sem=recv.at[number],
            device_id=device, device_id_type=MESH,
        )
        made.start()
        started.append(made)
        return made

    def spot(piece, *values):
        rows, cols, turn = piece
        return mine.at[(*at_groups(turn, *values), rows, cols)]

    waiting = [[] for _ in pieces]
    for phase in range(3):
        for n, piece in enumerate(pieces):
            turn = piece[2]
            q = [place.q[(turn + k) % 3] for k in range(3)]
            for made in waiting[n]:
                made.wait_recv()
            waiting[n] = []
            held = (q, q[:2], q[:1])[phase]
            group = (turn + 2 - phase) % 3
            block = spot(piece, *held)
            for flip in (1, 2, 3):
                number = base + (n * 3 + phase) * 3 + flip - 1
                waiting[n].append(copy(block, block, number, place.partner(group, flip)))
    first = base + 9 * len(pieces)
    across = []
    for n, piece in enumerate(pieces):
        turn = piece[2]
        own = place.q[turn]
        block = spot(piece, own)
        across.append(copy(block, block, first + 4 * n, place.other_core()))
    for n, piece in enumerate(pieces):
        turn = piece[2]
        for flip in (1, 2, 3):
            waiting[n][flip - 1].wait_recv()
            block = spot(piece, place.flipped(turn, flip))
            across.append(copy(block, block, first + 4 * n + flip, place.other_core()))
    for made in across:
        made.wait_recv()
    for made in started:
        made.wait_send()


def data_kernel(pieces, data_ref, out_ref, local_sem, send_sem, recv_sem):
    place = Place()
    rows = out_ref.shape[4]
    start = pl.multiple_of(place.row * rows, rows)
    unit = out_ref.at[(place.core, *place.q)]
    bring = pltpu.make_async_copy(data_ref.at[pl.ds(start, rows)], unit, local_sem)
    bring.start()
    meet(place)
    bring.wait()
    gather_phases(place, out_ref, pieces, (send_sem, recv_sem), 0)


def gather_data(data_points):
    count, width = data_points.shape
    peers = lax.axis_size("row")
    rows = count // peers
    quarter, tile = rows // 4, width // 4
    every = slice(None)
    last = slice(3 * quarter, rows)
    pieces = (
        (slice(0, quarter), every, 0),
        (slice(quarter, 2 * quarter), every, 1),
        (slice(2 * quarter, 3 * quarter), every, 2),
        (last, slice(0, tile), 0),
        (last, slice(tile, 2 * tile), 1),
        (last, slice(2 * tile, width), 2),
    )
    copies = 13 * len(pieces)
    out = pl.pallas_call(
        functools.partial(data_kernel, pieces),
        out_shape=jax.ShapeDtypeStruct((2, 4, 4, 4, rows, width), data_points.dtype),
        in_specs=[pl.BlockSpec(memory_space=pl.ANY)],
        out_specs=pl.BlockSpec(memory_space=pltpu.VMEM),
        scratch_shapes=[
            pltpu.SemaphoreType.DMA,
            pltpu.SemaphoreType.DMA((copies,)),
            pltpu.SemaphoreType.DMA((copies,)),
        ],
        compiler_params=pltpu.CompilerParams(
            collective_id=1, has_side_effects=True, vmem_limit_bytes=VMEM_CAP
        ),
        name="gather_data",
    )(data_points)
    return out.reshape(-1, width)


def join_pairs(first, second):
    peak = jnp.maximum(first[0], second[0])
    total = first[1] * jnp.exp(first[0] - peak) + second[1] * jnp.exp(second[0] - peak)
    return peak, total


def columns_kernel(in_ref, out_ref, held, slots, from_core, send_sem, recv_sem):
    place = Place()
    core = place.core
    meet(place)

    def copy(src, dst, number, device):
        made = pltpu.make_async_remote_copy(
            src_ref=src, dst_ref=dst, send_sem=send_sem.at[number], recv_sem=recv_sem.at[number],
            device_id=device, device_id_type=MESH,
        )
        made.start()
        return made

    other = 1 - core
    started = [copy(in_ref.at[other], from_core, 0, place.other_core())]
    started[0].wait_recv()
    own = in_ref[core]
    got = from_core[...]
    pair = join_pairs((own[0], own[1]), (got[0], got[1]))
    for group in range(3):
        held[group, 0] = pair[0]
        held[group, 1] = pair[1]
        now = [
            copy(held.at[group], slots.at[group, flip - 1], 3 * group + flip,
                 place.partner(group, flip))
            for flip in (1, 2, 3)
        ]
        started += now
        for flip in (1, 2, 3):
            now[flip - 1].wait_recv()
        new_peak = pair[0]
        for k in range(3):
            new_peak = jnp.maximum(new_peak, slots[group, k, 0])
        total = pair[1] * jnp.exp(pair[0] - new_peak)
        for k in range(3):
            total = total + slots[group, k, 1] * jnp.exp(slots[group, k, 0] - new_peak)
        pair = (new_peak, total)
    out_ref[core, 0] = pair[0]
    out_ref[core, 1] = pair[1]
    final = copy(out_ref.at[core], out_ref.at[core], 10, place.other_core())
    started.append(final)
    final.wait_recv()
    for made in started:
        made.wait_send()


def join_columns(pairs):
    shape = pairs.shape
    return pl.pallas_call(
        columns_kernel,
        out_shape=jax.ShapeDtypeStruct(shape, pairs.dtype),
        in_specs=[pl.BlockSpec(memory_space=pltpu.VMEM)],
        out_specs=pl.BlockSpec(memory_space=pltpu.VMEM),
        scratch_shapes=[
            pltpu.VMEM((3, *shape[1:]), jnp.float32),
            pltpu.VMEM((3, 3, *shape[1:]), jnp.float32),
            pltpu.VMEM(shape[1:], jnp.float32),
            pltpu.SemaphoreType.DMA((11,)),
            pltpu.SemaphoreType.DMA((11,)),
        ],
        compiler_params=pltpu.CompilerParams(collective_id=2, has_side_effects=True),
        name="join_columns",
    )(pairs)


def grads_kernel(pieces, in_ref, out_ref, acc, from_core, slot_0, slot_1, slot_2, send_sem, recv_sem):
    place = Place()
    core = place.core
    meet(place)
    count = len(pieces)

    def copy(src, dst, number, device):
        made = pltpu.make_async_remote_copy(
            src_ref=src, dst_ref=dst, send_sem=send_sem.at[number], recv_sem=recv_sem.at[number],
            device_id=device, device_id_type=MESH,
        )
        made.start()
        return made

    every = slice(None)
    other = 1 - core
    started = []
    first = []
    for n, (rows, cols, turn) in enumerate(pieces):
        made = copy(in_ref.at[other, :, :, :, :, cols], from_core.at[:, :, :, :, cols], n,
                    place.other_core())
        first.append(made)
    started += first
    base = count
    waiting = [[] for _ in pieces]
    for n, (rows, cols, turn) in enumerate(pieces):
        first[n].wait_recv()

        @pl.loop(0, 16)
        def _(i, cols=cols):
            a, b = i // 4, i % 4
            acc[a, b, :, :, cols] = in_ref[core, a, b, :, :, cols] + from_core[a, b, :, :, cols]

        for flip in (1, 2, 3):
            src = acc.at[(*at_groups(turn, place.flipped(turn, flip)), every, cols)]
            waiting[n].append(
                copy(src, slot_0.at[n, flip - 1, :, :, :, 0 : cols.stop - cols.start],
                     base + n * 3 + flip - 1, place.partner(turn, flip))
            )
    base += 3 * count
    for phase in (1, 2):
        for n, (rows, cols, turn) in enumerate(pieces):
            wide = slice(0, cols.stop - cols.start)
            q = [place.q[(turn + k) % 3] for k in range(3)]
            for made in waiting[n]:
                made.wait_recv()
            started += waiting[n]
            waiting[n] = []
            group = (turn + phase) % 3
            if phase == 1:
                lead = at_groups(turn, q[0])
                acc[(*lead, every, cols)] = (
                    (acc[(*lead, every, cols)] + slot_0[n, 0, :, :, :, wide])
                    + (slot_0[n, 1, :, :, :, wide] + slot_0[n, 2, :, :, :, wide])
                )
            else:
                lead = at_groups(turn, q[0], q[1])
                acc[(*lead, every, cols)] = (
                    (acc[(*lead, every, cols)] + slot_1[n, 0, :, :, wide])
                    + (slot_1[n, 1, :, :, wide] + slot_1[n, 2, :, :, wide])
                )
            for flip in (1, 2, 3):
                theirs = place.flipped(group, flip)
                if phase == 1:
                    src = acc.at[(*at_groups(turn, q[0], theirs), every, cols)]
                    dst = slot_1.at[n, flip - 1, :, :, wide]
                else:
                    src = acc.at[(*at_groups(turn, q[0], q[1], theirs), every, cols)]
                    dst = slot_2.at[n, flip - 1, :, wide]
                waiting[n].append(
                    copy(src, dst, base + n * 3 + flip - 1, place.partner(group, flip))
                )
        base += 3 * count
    for n, (rows, cols, turn) in enumerate(pieces):
        wide = slice(0, cols.stop - cols.start)
        for made in waiting[n]:
            made.wait_recv()
        started += waiting[n]
        out_ref[(core, *place.q, every, cols)] = (
            (acc[(*place.q, every, cols)] + slot_2[n, 0, :, wide])
            + (slot_2[n, 1, :, wide] + slot_2[n, 2, :, wide])
        )
    gather_phases(place, out_ref, pieces, (send_sem, recv_sem), base)
    for made in started:
        made.wait_send()


def sum_grads(grads):
    shape = grads.shape
    width = shape[-1]
    share = 128 * -(-width // 384)
    every = slice(None)
    pieces = (
        (every, slice(0, share), 0),
        (every, slice(share, 2 * share), 1),
        (every, slice(2 * share, width), 2),
    )
    copies = (1 + 9 + 13) * len(pieces)
    f32 = jnp.float32
    return pl.pallas_call(
        functools.partial(grads_kernel, pieces),
        out_shape=jax.ShapeDtypeStruct(shape, f32),
        in_specs=[pl.BlockSpec(memory_space=pltpu.VMEM)],
        out_specs=pl.BlockSpec(memory_space=pltpu.VMEM),
        scratch_shapes=[
            pltpu.VMEM(shape[1:], f32),
            pltpu.VMEM(shape[1:], f32),
            pltpu.VMEM((3, 3, 4, 4, 8, share), f32),
            pltpu.VMEM((3, 3, 4, 8, share), f32),
            pltpu.VMEM((3, 3, 8, share), f32),
            pltpu.SemaphoreType.DMA((copies,)),
            pltpu.SemaphoreType.DMA((copies,)),
        ],
        compiler_params=pltpu.CompilerParams(
            collective_id=3, has_side_effects=True, vmem_limit_bytes=VMEM_CAP
        ),
        name="sum_grads",
    )(grads)


def on_device(noise_points, data_points, times, time_shift, weight_in, weight_out):
    count_row = lax.axis_size("row")
    count_col = lax.axis_size("col")
    rows_here = noise_points.shape[0]
    total_noise = rows_here * count_row
    total_data = data_points.shape[0] * count_col
    width = noise_points.shape[1]
    share = rows_here // count_col
    steps_each = times.shape[1]

    data_all = gather_data(data_points)
    anchor = lax.dynamic_slice_in_dim(noise_points, lax.axis_index("col") * share, share, 0)
    noise_sq = jnp.sum(anchor * anchor, axis=1)
    data_sq = jnp.sum(data_all * data_all, axis=1)
    inner = lax.dot_general(
        anchor, data_all, (((1,), (1,)), ((), ())), precision=HIGH_PREC,
        preferred_element_type=jnp.float32,
    )
    cost = (noise_sq[:, None] + data_sq[None, :] - 2.0 * inner) / width
    scores = -cost / ENTROPY
    row_peak = jnp.max(scores, axis=1)
    row_total = jnp.sum(jnp.exp(scores - row_peak[:, None]), axis=1)
    potential_f = -ENTROPY * (row_peak + jnp.log(row_total) - math.log(float(total_data)))
    scores = (potential_f[:, None] - cost) / ENTROPY
    local_peak = jnp.max(scores, axis=0)
    local_total = jnp.sum(jnp.exp(scores - local_peak[None, :]), axis=0)
    pairs = jnp.stack(
        [local_peak.reshape(2, -1, 128), local_total.reshape(2, -1, 128)], axis=1
    )
    joined = join_columns(pairs)
    col_peak, col_total = joined[:, 0].reshape(-1), joined[:, 1].reshape(-1)
    potential_g = -ENTROPY * (col_peak + jnp.log(col_total) - math.log(float(total_noise)))
    scores = (potential_g[None, :] - cost) / ENTROPY
    final_peak = jnp.max(scores, axis=1)
    weights = jnp.exp(scores - final_peak[:, None])
    numer = jnp.dot(weights, data_all, precision=HIGH_PREC, preferred_element_type=jnp.float32)
    target = numer / jnp.sum(weights, axis=1)[:, None]

    tvals = times[:, :, None]
    mixed = (
        ((1.0 - tvals) * anchor[:, None, :] + tvals * target[:, None, :])
        .reshape(share * steps_each, width)
        .astype(jnp.bfloat16)
    )
    velocity = jnp.broadcast_to((target - anchor)[:, None, :], (share, steps_each, width)).reshape(
        share * steps_each, width
    )
    hid_width = weight_in.shape[1]
    pre = (
        jnp.dot(mixed, weight_in, preferred_element_type=jnp.float32)
        + times.reshape(share * steps_each, 1) * time_shift[None, :]
    )
    hidden = jax.nn.silu(pre).astype(jnp.bfloat16)
    output = jnp.dot(hidden, weight_out, preferred_element_type=jnp.float32)
    predicted = output.astype(jnp.bfloat16)
    scale = 1.0 / math.sqrt(float(total_noise * steps_each))
    delta = ((output - velocity) * scale).astype(jnp.bfloat16)
    back = lax.dot_general(
        delta, weight_out, (((1,), (1,)), ((), ())), preferred_element_type=jnp.float32
    )
    sig = jax.nn.sigmoid(pre)
    delta_pre = (back * sig * (1.0 + pre * (1.0 - sig))).astype(jnp.bfloat16)
    contract = (((0,), (0,)), ((), ()))
    first = lax.dot_general(mixed, delta_pre, contract, preferred_element_type=jnp.float32)
    second = lax.dot_general(hidden, delta, contract, preferred_element_type=jnp.float32)
    halves = hid_width // width
    second = jnp.concatenate(
        [second[k * width : (k + 1) * width] for k in range(halves)], axis=1
    )
    grads = jnp.stack([first, second]).reshape(2, 4, 4, 4, width // 64, hid_width)
    summed = sum_grads(grads).reshape(2, width, hid_width)
    grad_in = summed[0]
    grad_out = jnp.concatenate(
        [summed[1][:, k * width : (k + 1) * width] for k in range(halves)], axis=0
    )
    return (predicted, grad_in, grad_out)


def solution(mesh):
    in_specs = (P("row", None), P("col", None), P(("row", "col"), None), P(), P(), P())
    out_specs = (P(("row", "col"), None), P(), P())
    return jax.shard_map(
        on_device, mesh=mesh, in_specs=in_specs, out_specs=out_specs, check_vma=False
    )
```

```python
import functools
import math

import jax
import jax.numpy as jnp
from jax import lax
from jax.experimental import pallas as pl
from jax.experimental.pallas import tpu as pltpu
from jax.sharding import PartitionSpec as P

ENTROPY = 0.05
MESH = pl.DeviceIdType.MESH
VMEM_CAP = 60 * 1024 * 1024


class Place:
    def __init__(self):
        row, col = lax.axis_index("row"), lax.axis_index("col")
        self.core = col % 2
        x = (row % 2) * 2 + (col // 2) % 2
        y = row // 2
        z = col // 4
        self.bits = []
        for pos in (x, y, z):
            self.bits.append(((pos + pos // 2) % 2, pos // 2))
        (xa, xb), (ya, yb), (za, zb) = self.bits
        self.groups = ((xa, ya), (yb, za), (zb, xb))
        self.q = tuple(u * 2 + v for u, v in self.groups)
        self.row, self.col = row, col

    def partner(self, group, flip, cross=0):
        hi, lo = flip // 2, flip % 2
        core = 1 - self.core if cross else self.core
        groups = [list(g) for g in self.groups]
        if hi:
            groups[group][0] = 1 - groups[group][0]
        if lo:
            groups[group][1] = 1 - groups[group][1]
        (xa, ya), (yb, za), (zb, xb) = groups
        x, y, z = ((2 * b + (a + b) % 2) for a, b in ((xa, xb), (ya, yb), (za, zb)))
        return (y * 2 + x // 2, z * 4 + (x % 2) * 2 + core)

    def other_core(self):
        return (self.row, self.col + 1 - 2 * self.core)

    def flipped(self, group, flip):
        hi, lo = self.groups[group]
        if flip // 2:
            hi = 1 - hi
        if flip % 2:
            lo = 1 - lo
        return hi * 2 + lo


def meet(place):
    barrier = pltpu.get_barrier_semaphore()
    pl.semaphore_signal(barrier, inc=1, device_id=place.other_core(), device_id_type=MESH)
    for group in range(3):
        for flip in (1, 2, 3):
            pl.semaphore_signal(
                barrier, inc=1, device_id=place.partner(group, flip), device_id_type=MESH
            )
    pl.semaphore_wait(barrier, 10)


def at_groups(turn, first=None, second=None, third=None):
    found = [slice(None)] * 3
    for k, value in enumerate((first, second, third)):
        if value is not None:
            found[(turn + k) % 3] = value
    return tuple(found)


def gather_phases(place, out, pieces, sems, base):
    send, recv = sems
    mine = out.at[place.core]
    started = []

    def copy(src, dst, number, device):
        made = pltpu.make_async_remote_copy(
            src_ref=src, dst_ref=dst, send_sem=send.at[number], recv_sem=recv.at[number],
            device_id=device, device_id_type=MESH,
        )
        made.start()
        started.append(made)
        return made

    def spot(piece, *values):
        rows, cols, turn = piece
        return mine.at[(*at_groups(turn, *values), rows, cols)]

    waiting = [[] for _ in pieces]
    for phase in range(3):
        for n, piece in enumerate(pieces):
            turn = piece[2]
            q = [place.q[(turn + k) % 3] for k in range(3)]
            for made in waiting[n]:
                made.wait_recv()
            waiting[n] = []
            held = (q, q[:2], q[:1])[phase]
            group = (turn + 2 - phase) % 3
            block = spot(piece, *held)
            for flip in (1, 2, 3):
                number = base + (n * 3 + phase) * 3 + flip - 1
                waiting[n].append(copy(block, block, number, place.partner(group, flip)))
    first = base + 9 * len(pieces)
    across = []
    for n, piece in enumerate(pieces):
        turn = piece[2]
        own = place.q[turn]
        block = spot(piece, own)
        across.append(copy(block, block, first + 4 * n, place.other_core()))
    for n, piece in enumerate(pieces):
        turn = piece[2]
        for flip in (1, 2, 3):
            waiting[n][flip - 1].wait_recv()
            block = spot(piece, place.flipped(turn, flip))
            across.append(copy(block, block, first + 4 * n + flip, place.other_core()))
    for made in across:
        made.wait_recv()
    for made in started:
        made.wait_send()


def meet_all(place):
    barrier = pltpu.get_barrier_semaphore()
    known = [place.other_core()]
    for group, both in ((0, True), (1, False), (2, True)):
        for flip in (1, 2, 3):
            known.append(place.partner(group, flip))
            if both:
                known.append(place.partner(group, flip, 1))
    for device in known:
        pl.semaphore_signal(barrier, inc=1, device_id=device, device_id_type=MESH)
    pl.semaphore_wait(barrier, len(known))


def joined(pairs):
    peak = pairs[0][0]
    for other, _ in pairs[1:]:
        peak = jnp.maximum(peak, other)
    total = pairs[0][1] * jnp.exp(pairs[0][0] - peak)
    for other, amount in pairs[1:]:
        total = total + amount * jnp.exp(other - peak)
    return peak, total


def join_columns(place, pairs, held, slots, send, recv, base):
    core = place.core
    started = []

    def copy(src, dst, number, device):
        made = pltpu.make_async_remote_copy(
            src_ref=src, dst_ref=dst, send_sem=send.at[number], recv_sem=recv.at[number],
            device_id=device, device_id_type=MESH,
        )
        made.start()
        started.append(made)
        return made

    def device(group, flip, cross):
        return place.other_core() if flip == 0 else place.partner(group, flip, cross)

    ways = [(flip, cross) for flip in range(4) for cross in range(2) if flip or cross]
    now = []
    for flip, cross in ways:
        k = 2 * flip + cross
        half = 1 - core if cross else core
        now.append(copy(pairs.at[half], slots.at[0, k], base + k, device(0, flip, cross)))
    for made in now:
        made.wait_recv()
    found = [(pairs[core, 0], pairs[core, 1])]
    found += [(slots[0, 2 * f + c, 0], slots[0, 2 * f + c, 1]) for f, c in ways]
    held[0, 0], held[0, 1] = joined(found)
    now = []
    for flip in (1, 2, 3):
        number = base + 8 + flip
        now.append(copy(held.at[0], slots.at[1, flip], number, device(1, flip, 0)))
    for made in now:
        made.wait_recv()
    found = [(held[0, 0], held[0, 1])]
    found += [(slots[1, flip, 0], slots[1, flip, 1]) for flip in (1, 2, 3)]
    held[1, 0], held[1, 1] = joined(found)
    now = []
    for flip, cross in ways:
        k = 2 * flip + cross
        now.append(copy(held.at[1], slots.at[2, k], base + 16 + k, device(2, flip, cross)))
    for made in now:
        made.wait_recv()
    found = [(held[1, 0], held[1, 1])]
    found += [(slots[2, 2 * flip, 0], slots[2, 2 * flip, 1]) for flip in (1, 2, 3)]
    own = joined(found)
    other = joined([(slots[2, 2 * flip + 1, 0], slots[2, 2 * flip + 1, 1]) for flip in range(4)])
    return own, other, started


def target_kernel(
    pieces, total_noise, data_ref, noise_ref, target_ref, data, data_hi, data_lo, anchor, anchor_hi,
    anchor_lo, score, running, pairs, held, slots, local_sem, send_sem, recv_sem,
):
    place = Place()
    f32, bf16 = jnp.float32, jnp.bfloat16
    rows = data.shape[4]
    share, width = anchor.shape
    chunks, _, chunk = score.shape
    total_data = chunks * chunk
    start = pl.multiple_of(place.row * rows, rows)
    unit = data.at[(place.core, *place.q)]
    bring = pltpu.make_async_copy(data_ref.at[pl.ds(start, rows)], unit, local_sem.at[0])
    bring.start()
    first = pl.multiple_of(place.col * share, share)
    noise = pltpu.make_async_copy(noise_ref.at[pl.ds(first, share)], anchor, local_sem.at[1])
    noise.start()
    meet_all(place)
    bring.wait()
    noise.wait()
    x = anchor[...]
    high = x.astype(bf16)
    anchor_hi[...] = high
    anchor_lo[...] = (x - high.astype(f32)).astype(bf16)
    noise_sq = jnp.sum(x * x, axis=1, keepdims=True)
    gather_phases(place, data, pieces, (send_sem, recv_sem), 0)

    across = (((1,), (1,)), ((), ()))
    lanes = 128
    tiles = chunk // lanes
    running[...] = jnp.full_like(running, -jnp.inf)

    @pl.loop(0, chunks)
    def _(i):
        points = data[i // 8, (i // 2) % 4, pl.ds((i % 2) * 2, 2)].reshape(chunk, width)
        high = points.astype(bf16)
        low = (points - high.astype(f32)).astype(bf16)
        data_hi[i] = high
        data_lo[i] = low
        square = points * points
        part = square[:, :lanes]
        for k in range(1, width // lanes):
            part = part + square[:, k * lanes : (k + 1) * lanes]
        data_sq = jnp.sum(part.T, axis=0, keepdims=True)
        inner = lax.dot_general(anchor_hi[...], high, across, preferred_element_type=f32)
        inner += lax.dot_general(anchor_hi[...], low, across, preferred_element_type=f32)
        inner += lax.dot_general(anchor_lo[...], high, across, preferred_element_type=f32)
        cost = (noise_sq + data_sq - 2.0 * inner) * (1.0 / width)
        found = cost * (-1.0 / ENTROPY)
        score[i] = found
        peak = running[...]
        for k in range(tiles):
            peak = jnp.maximum(peak, found[:, k * lanes : (k + 1) * lanes])
        running[...] = peak

    peak = jnp.max(running[...], axis=1, keepdims=True)
    running[...] = jnp.zeros_like(running)

    @pl.loop(0, chunks)
    def _(i):
        e = jnp.exp(score[i] - peak)
        total = running[...]
        for k in range(tiles):
            total = total + e[:, k * lanes : (k + 1) * lanes]
        running[...] = total

    total = jnp.sum(running[...], axis=1, keepdims=True)
    row_lse = peak + jnp.log(total) - math.log(float(total_data))

    @pl.loop(0, chunks)
    def _(i):
        s = score[i] - row_lse
        col_peak = jnp.max(s, axis=0, keepdims=True)
        col_total = jnp.sum(jnp.exp(s - col_peak), axis=0, keepdims=True)
        for k in range(tiles):
            at = i * tiles + k
            cols = slice(k * lanes, (k + 1) * lanes)
            pairs[at // 16, 0, pl.ds(at % 16, 1), :] = col_peak[:, cols]
            pairs[at // 16, 1, pl.ds(at % 16, 1), :] = col_total[:, cols]

    base = 13 * len(pieces)
    own, other, started = join_columns(place, pairs, held, slots, send_sem, recv_sem, base)
    for made in started:
        made.wait_send()
    log_noise = math.log(float(total_noise))
    pairs[place.core, 0] = own[0] + jnp.log(own[1]) - log_noise
    pairs[1 - place.core, 0] = other[0] + jnp.log(other[1]) - log_noise
    running[...] = jnp.full_like(running, -jnp.inf)

    @pl.loop(0, chunks)
    def _(i):
        peak = running[...]
        for k in range(tiles):
            at = i * tiles + k
            cols = slice(k * lanes, (k + 1) * lanes)
            s = score[i, :, cols] - pairs[at // 16, 0, pl.ds(at % 16, 1), :]
            score[i, :, cols] = s
            peak = jnp.maximum(peak, s)
        running[...] = peak

    peak = jnp.max(running[...], axis=1, keepdims=True)
    running[...] = jnp.zeros_like(running)
    target_ref[...] = jnp.zeros_like(target_ref)

    @pl.loop(0, chunks)
    def _(i):
        weights = jnp.exp(score[i] - peak).astype(bf16)
        total = running[...]
        for k in range(tiles):
            total = total + weights[:, k * lanes : (k + 1) * lanes].astype(f32)
        running[...] = total
        target_ref[...] += jnp.dot(
            weights, data_hi[i], preferred_element_type=f32
        ) + jnp.dot(weights, data_lo[i], preferred_element_type=f32)

    target_ref[...] = target_ref[...] / jnp.sum(running[...], axis=1, keepdims=True)


def find_target(noise_points, data_points, total_noise, share):
    count, width = data_points.shape
    peers = lax.axis_size("row")
    rows = count // peers
    total_data = count * lax.axis_size("col")
    quarter, tile = rows // 4, width // 4
    every = slice(None)
    last = slice(3 * quarter, rows)
    pieces = (
        (slice(0, quarter), every, 0),
        (slice(quarter, 2 * quarter), every, 1),
        (slice(2 * quarter, 3 * quarter), every, 2),
        (last, slice(0, tile), 0),
        (last, slice(tile, 2 * tile), 1),
        (last, slice(2 * tile, width), 2),
    )
    copies = 13 * len(pieces) + 24
    chunk = 8 * rows
    chunks = total_data // chunk
    f32, bf16 = jnp.float32, jnp.bfloat16
    half = (2, total_data // 256, 128)
    return pl.pallas_call(
        functools.partial(target_kernel, pieces, total_noise),
        out_shape=jax.ShapeDtypeStruct((share, width), f32),
        in_specs=[pl.BlockSpec(memory_space=pl.ANY)] * 2,
        out_specs=pl.BlockSpec(memory_space=pltpu.VMEM),
        scratch_shapes=[
            pltpu.VMEM((2, 4, 4, 4, rows, width), f32),
            pltpu.VMEM((chunks, chunk, width), bf16),
            pltpu.VMEM((chunks, chunk, width), bf16),
            pltpu.VMEM((share, width), f32),
            pltpu.VMEM((share, width), bf16),
            pltpu.VMEM((share, width), bf16),
            pltpu.VMEM((chunks, share, chunk), f32),
            pltpu.VMEM((share, 128), f32),
            pltpu.VMEM((2, *half), f32),
            pltpu.VMEM((2, *half), f32),
            pltpu.VMEM((3, 8, *half), f32),
            pltpu.SemaphoreType.DMA((2,)),
            pltpu.SemaphoreType.DMA((copies,)),
            pltpu.SemaphoreType.DMA((copies,)),
        ],
        compiler_params=pltpu.CompilerParams(
            collective_id=1, has_side_effects=True, vmem_limit_bytes=VMEM_CAP
        ),
        name="find_target",
    )(data_points, noise_points)


def grads_kernel(pieces, in_ref, out_ref, acc, from_core, slot_0, slot_1, slot_2, send_sem, recv_sem):
    place = Place()
    core = place.core
    meet(place)
    count = len(pieces)

    def copy(src, dst, number, device):
        made = pltpu.make_async_remote_copy(
            src_ref=src, dst_ref=dst, send_sem=send_sem.at[number], recv_sem=recv_sem.at[number],
            device_id=device, device_id_type=MESH,
        )
        made.start()
        return made

    every = slice(None)
    other = 1 - core
    started = []
    first = []
    for n, (rows, cols, turn) in enumerate(pieces):
        made = copy(in_ref.at[other, :, :, :, :, cols], from_core.at[:, :, :, :, cols], n,
                    place.other_core())
        first.append(made)
    started += first
    base = count
    waiting = [[] for _ in pieces]
    for n, (rows, cols, turn) in enumerate(pieces):
        first[n].wait_recv()

        @pl.loop(0, 16)
        def _(i, cols=cols):
            a, b = i // 4, i % 4
            acc[a, b, :, :, cols] = in_ref[core, a, b, :, :, cols] + from_core[a, b, :, :, cols]

        for flip in (1, 2, 3):
            src = acc.at[(*at_groups(turn, place.flipped(turn, flip)), every, cols)]
            waiting[n].append(
                copy(src, slot_0.at[n, flip - 1, :, :, :, 0 : cols.stop - cols.start],
                     base + n * 3 + flip - 1, place.partner(turn, flip))
            )
    base += 3 * count
    for phase in (1, 2):
        for n, (rows, cols, turn) in enumerate(pieces):
            wide = slice(0, cols.stop - cols.start)
            q = [place.q[(turn + k) % 3] for k in range(3)]
            for made in waiting[n]:
                made.wait_recv()
            started += waiting[n]
            waiting[n] = []
            group = (turn + phase) % 3
            if phase == 1:
                lead = at_groups(turn, q[0])
                acc[(*lead, every, cols)] = (
                    (acc[(*lead, every, cols)] + slot_0[n, 0, :, :, :, wide])
                    + (slot_0[n, 1, :, :, :, wide] + slot_0[n, 2, :, :, :, wide])
                )
            else:
                lead = at_groups(turn, q[0], q[1])
                acc[(*lead, every, cols)] = (
                    (acc[(*lead, every, cols)] + slot_1[n, 0, :, :, wide])
                    + (slot_1[n, 1, :, :, wide] + slot_1[n, 2, :, :, wide])
                )
            for flip in (1, 2, 3):
                theirs = place.flipped(group, flip)
                if phase == 1:
                    src = acc.at[(*at_groups(turn, q[0], theirs), every, cols)]
                    dst = slot_1.at[n, flip - 1, :, :, wide]
                else:
                    src = acc.at[(*at_groups(turn, q[0], q[1], theirs), every, cols)]
                    dst = slot_2.at[n, flip - 1, :, wide]
                waiting[n].append(
                    copy(src, dst, base + n * 3 + flip - 1, place.partner(group, flip))
                )
        base += 3 * count
    for n, (rows, cols, turn) in enumerate(pieces):
        wide = slice(0, cols.stop - cols.start)
        for made in waiting[n]:
            made.wait_recv()
        started += waiting[n]
        out_ref[(core, *place.q, every, cols)] = (
            (acc[(*place.q, every, cols)] + slot_2[n, 0, :, wide])
            + (slot_2[n, 1, :, wide] + slot_2[n, 2, :, wide])
        )
    gather_phases(place, out_ref, pieces, (send_sem, recv_sem), base)
    for made in started:
        made.wait_send()


def sum_grads(grads):
    shape = grads.shape
    width = shape[-1]
    share = 128 * -(-width // 384)
    every = slice(None)
    pieces = (
        (every, slice(0, share), 0),
        (every, slice(share, 2 * share), 1),
        (every, slice(2 * share, width), 2),
    )
    copies = (1 + 9 + 13) * len(pieces)
    f32 = jnp.float32
    return pl.pallas_call(
        functools.partial(grads_kernel, pieces),
        out_shape=jax.ShapeDtypeStruct(shape, f32),
        in_specs=[pl.BlockSpec(memory_space=pltpu.VMEM)],
        out_specs=pl.BlockSpec(memory_space=pltpu.VMEM),
        scratch_shapes=[
            pltpu.VMEM(shape[1:], f32),
            pltpu.VMEM(shape[1:], f32),
            pltpu.VMEM((3, 3, 4, 4, 8, share), f32),
            pltpu.VMEM((3, 3, 4, 8, share), f32),
            pltpu.VMEM((3, 3, 8, share), f32),
            pltpu.SemaphoreType.DMA((copies,)),
            pltpu.SemaphoreType.DMA((copies,)),
        ],
        compiler_params=pltpu.CompilerParams(
            collective_id=3, has_side_effects=True, vmem_limit_bytes=VMEM_CAP
        ),
        name="sum_grads",
    )(grads)


def spread(rows, steps_each):
    count, width = rows.shape
    wide = jnp.broadcast_to(rows[:, None, :], (count, steps_each, width))
    return wide.reshape(count * steps_each, width)


def train_kernel(
    scale, points, steps_each, anchor_ref, target_ref, tvals_ref, shift_ref, w_in_ref, w_out_ref,
    w_back_ref, predicted_ref, grads_ref, mixed_ref, hidden_ref, delta_ref, delta_pre_ref,
):
    block = points * steps_each
    width, hid_width = w_in_ref.shape
    blocks = anchor_ref.shape[0] // points
    grads_ref[...] = jnp.zeros_like(grads_ref)
    f32, bf16 = jnp.float32, jnp.bfloat16
    contract = (((0,), (0,)), ((), ()))
    lanes = 128

    def forward(b, slot):
        here = pl.ds(pl.multiple_of(b * points, points), points)
        anchor, target = anchor_ref[here, :], target_ref[here, :]
        tvals = tvals_ref[pl.ds(pl.multiple_of(b * block, block), block), :]
        parts = []
        for k in range(width // lanes):
            cols = slice(k * lanes, (k + 1) * lanes)
            x, y = spread(anchor[:, cols], steps_each), spread(target[:, cols], steps_each)
            parts.append(((1.0 - tvals) * x + tvals * y).astype(bf16))
        mixed = jnp.concatenate(parts, axis=1)
        mixed_ref[slot] = mixed
        pre = jnp.dot(mixed, w_in_ref[...], preferred_element_type=f32)
        shift = jnp.concatenate(
            [tvals * shift_ref[:, k * lanes : (k + 1) * lanes] for k in range(hid_width // lanes)],
            axis=1,
        )
        pre = pre + shift
        sig = 0.5 * jnp.tanh(0.5 * pre) + 0.5
        hidden = (pre * sig).astype(bf16)
        slope = sig * (1.0 + pre * (1.0 - sig))
        hidden_ref[slot] = hidden
        output = jnp.dot(hidden, w_out_ref[...], preferred_element_type=f32)
        predicted_ref[pl.ds(pl.multiple_of(b * block, block), block), :] = output.astype(bf16)
        velocity = spread(target - anchor, steps_each)
        delta = ((output - velocity) * scale).astype(bf16)
        delta_ref[slot] = delta
        back = jnp.dot(delta, w_back_ref[...], preferred_element_type=f32)
        delta_pre_ref[slot] = (back * slope).astype(bf16)

    def add_grads(slot):
        grads_ref[0] += lax.dot_general(
            mixed_ref[slot], delta_pre_ref[slot], contract, preferred_element_type=f32
        )
        for k in range(hid_width // width):
            cols = slice(k * width, (k + 1) * width)
            grads_ref[1, :, cols] += lax.dot_general(
                hidden_ref[slot, :, cols], delta_ref[slot], contract, preferred_element_type=f32
            )

    forward(0, 0)

    @pl.loop(1, blocks)
    def _(b):
        forward(b, b % 2)
        add_grads((b + 1) % 2)

    add_grads((blocks - 1) % 2)


def train(anchor, target, times, time_shift, weight_in, weight_out, scale):
    share, width = anchor.shape
    hid_width = weight_in.shape[1]
    steps_each = times.shape[1]
    points = 32
    block = points * steps_each
    tvals = jnp.broadcast_to(times.reshape(share * steps_each, 1), (share * steps_each, 128))
    bf16 = jnp.bfloat16
    vmem = pl.BlockSpec(memory_space=pltpu.VMEM)
    return pl.pallas_call(
        functools.partial(train_kernel, scale, points, steps_each),
        out_shape=(
            jax.ShapeDtypeStruct((share * steps_each, width), bf16),
            jax.ShapeDtypeStruct((2, width, hid_width), jnp.float32),
        ),
        in_specs=[vmem] * 7,
        out_specs=(vmem, vmem),
        scratch_shapes=[
            pltpu.VMEM((2, block, width), bf16),
            pltpu.VMEM((2, block, hid_width), bf16),
            pltpu.VMEM((2, block, width), bf16),
            pltpu.VMEM((2, block, hid_width), bf16),
        ],
        compiler_params=pltpu.CompilerParams(vmem_limit_bytes=VMEM_CAP),
        name="train",
    )(anchor, target, tvals, time_shift.reshape(1, hid_width), weight_in, weight_out, weight_out.T)


def on_device(noise_points, data_points, times, time_shift, weight_in, weight_out):
    count_row = lax.axis_size("row")
    count_col = lax.axis_size("col")
    rows_here = noise_points.shape[0]
    total_noise = rows_here * count_row
    width = noise_points.shape[1]
    share = rows_here // count_col
    steps_each = times.shape[1]

    target = find_target(noise_points, data_points, total_noise, share)
    anchor = lax.dynamic_slice_in_dim(noise_points, lax.axis_index("col") * share, share, 0)
    scale = 1.0 / math.sqrt(float(total_noise * steps_each))
    predicted, grads = train(
        anchor, target, times, time_shift, weight_in, weight_out, scale
    )
    hid_width = weight_in.shape[1]
    halves = hid_width // width
    grads = grads.reshape(2, 4, 4, 4, width // 64, hid_width)
    summed = sum_grads(grads).reshape(2, width, hid_width)
    grad_in = summed[0]
    grad_out = jnp.concatenate(
        [summed[1][:, k * width : (k + 1) * width] for k in range(halves)], axis=0
    )
    return (predicted, grad_in, grad_out)


def solution(mesh):
    in_specs = (P("row", None), P("col", None), P(("row", "col"), None), P(), P(), P())
    out_specs = (P(("row", "col"), None), P(), P())
    return jax.shard_map(
        on_device, mesh=mesh, in_specs=in_specs, out_specs=out_specs, check_vma=False
    )
```

```python
import functools
import math

import jax
import jax.numpy as jnp
from jax import lax
from jax.experimental import pallas as pl
from jax.experimental.pallas import tpu as pltpu
from jax.sharding import PartitionSpec as P

ENTROPY = 0.05
MESH = pl.DeviceIdType.MESH
VMEM_CAP = 60 * 1024 * 1024
GATHERS = 19


class Place:
    def __init__(self):
        row, col = lax.axis_index("row"), lax.axis_index("col")
        self.core = col % 2
        x = (row % 2) * 2 + (col // 2) % 2
        y = row // 2
        z = col // 4
        self.bits = []
        for pos in (x, y, z):
            self.bits.append(((pos + pos // 2) % 2, pos // 2))
        (xa, xb), (ya, yb), (za, zb) = self.bits
        self.groups = ((xa, ya), (yb, za), (zb, xb))
        self.q = tuple(u * 2 + v for u, v in self.groups)
        self.row, self.col = row, col

    def partner(self, group, flip, cross=0):
        hi, lo = flip // 2, flip % 2
        core = 1 - self.core if cross else self.core
        groups = [list(g) for g in self.groups]
        if hi:
            groups[group][0] = 1 - groups[group][0]
        if lo:
            groups[group][1] = 1 - groups[group][1]
        (xa, ya), (yb, za), (zb, xb) = groups
        x, y, z = ((2 * b + (a + b) % 2) for a, b in ((xa, xb), (ya, yb), (za, zb)))
        return (y * 2 + x // 2, z * 4 + (x % 2) * 2 + core)

    def other_core(self):
        return (self.row, self.col + 1 - 2 * self.core)

    def flipped(self, group, flip):
        hi, lo = self.groups[group]
        if flip // 2:
            hi = 1 - hi
        if flip % 2:
            lo = 1 - lo
        return hi * 2 + lo


def meet(place):
    barrier = pltpu.get_barrier_semaphore()
    pl.semaphore_signal(barrier, inc=1, device_id=place.other_core(), device_id_type=MESH)
    for group in range(3):
        for flip in (1, 2, 3):
            pl.semaphore_signal(
                barrier, inc=1, device_id=place.partner(group, flip), device_id_type=MESH
            )
    pl.semaphore_wait(barrier, 10)


def at_groups(turn, first=None, second=None, third=None):
    found = [slice(None)] * 3
    for k, value in enumerate((first, second, third)):
        if value is not None:
            found[(turn + k) % 3] = value
    return tuple(found)


def gather_phases(place, out, pieces, sems, base, phases=(0, 1, 2)):
    send, recv = sems
    mine = out.at[place.core]
    started = []

    def copy(block, number, device):
        made = pltpu.make_async_remote_copy(
            src_ref=block, dst_ref=block, send_sem=send.at[number], recv_sem=recv.at[number],
            device_id=device, device_id_type=MESH,
        )
        made.start()
        started.append(made)
        return made

    def spot(piece, *values):
        rows, cols, turn = piece
        return mine.at[(*at_groups(turn, *values), rows, cols)]

    waiting = [[] for _ in pieces]
    for phase in phases[:-1]:
        for n, piece in enumerate(pieces):
            turn = piece[2]
            q = [place.q[(turn + k) % 3] for k in range(3)]
            for made in waiting[n]:
                made.wait_recv()
            waiting[n] = []
            group = (turn + 2 - phase) % 3
            block = spot(piece, *(q, q[:2])[phase])
            for flip in (1, 2, 3):
                number = base + GATHERS * n + phase * 3 + flip - 1
                waiting[n].append(copy(block, number, place.partner(group, flip)))
    halves = (pl.ds(0, 2), pl.ds(2, 2))
    across, landed = [], []
    for n, piece in enumerate(pieces):
        turn = piece[2]
        for made in waiting[n]:
            made.wait_recv()
        first = base + GATHERS * n + 6
        own = place.q[turn]
        now = {}
        for k in range(2):
            for flip, half in ((2, k), (1, 1 - k)):
                block = spot(piece, own, halves[half])
                now[flip, half] = copy(block, first + 2 * (flip - 1) + half,
                                       place.partner(turn, flip))
        across.append(copy(spot(piece, own), first + 6, place.other_core()))
        landed.append(now)
    for flip, half, step in ((2, 0, 0), (1, 1, 0), (2, 1, 1), (1, 0, 1)):
        for n, piece in enumerate(pieces):
            turn = piece[2]
            first = base + GATHERS * n + 6
            landed[n][flip, half].wait_recv()
            block = spot(piece, place.flipped(turn, flip), halves[half])
            if step == 0:
                landed[n][3, half] = copy(block, first + 4 + half, place.partner(turn, 3 - flip))
            across.append(
                copy(block, first + 7 + 2 * (flip - 1) + half, place.other_core())
            )
    for half in range(2):
        for n, piece in enumerate(pieces):
            turn = piece[2]
            first = base + GATHERS * n + 6
            landed[n][3, half].wait_recv()
            block = spot(piece, place.flipped(turn, 3), halves[half])
            across.append(copy(block, first + 11 + half, place.other_core()))
    for made in across:
        made.wait_recv()
    for made in started:
        made.wait_send()


def meet_all(place):
    barrier = pltpu.get_barrier_semaphore()
    known = [place.other_core()]
    for group, both in ((0, True), (1, False), (2, True)):
        for flip in (1, 2, 3):
            known.append(place.partner(group, flip))
            if both:
                known.append(place.partner(group, flip, 1))
    for device in known:
        pl.semaphore_signal(barrier, inc=1, device_id=device, device_id_type=MESH)
    pl.semaphore_wait(barrier, len(known))


def joined(pairs):
    peak = pairs[0][0]
    for other, _ in pairs[1:]:
        peak = jnp.maximum(peak, other)
    total = pairs[0][1] * jnp.exp(pairs[0][0] - peak)
    for other, amount in pairs[1:]:
        total = total + amount * jnp.exp(other - peak)
    return peak, total


def join_columns(place, pairs, held, slots, send, recv, base):
    core = place.core
    started = []

    def copy(src, dst, number, device):
        made = pltpu.make_async_remote_copy(
            src_ref=src, dst_ref=dst, send_sem=send.at[number], recv_sem=recv.at[number],
            device_id=device, device_id_type=MESH,
        )
        made.start()
        started.append(made)
        return made

    def device(group, flip, cross):
        return place.other_core() if flip == 0 else place.partner(group, flip, cross)

    ways = [(flip, cross) for flip in range(4) for cross in range(2) if flip or cross]
    now = []
    for flip, cross in ways:
        k = 2 * flip + cross
        half = 1 - core if cross else core
        now.append(copy(pairs.at[half], slots.at[0, k], base + k, device(0, flip, cross)))
    for made in now:
        made.wait_recv()
    found = [(pairs[core, 0], pairs[core, 1])]
    found += [(slots[0, 2 * f + c, 0], slots[0, 2 * f + c, 1]) for f, c in ways]
    held[0, 0], held[0, 1] = joined(found)
    now = []
    for flip in (1, 2, 3):
        number = base + 8 + flip
        now.append(copy(held.at[0], slots.at[1, flip], number, device(1, flip, 0)))
    for made in now:
        made.wait_recv()
    found = [(held[0, 0], held[0, 1])]
    found += [(slots[1, flip, 0], slots[1, flip, 1]) for flip in (1, 2, 3)]
    held[1, 0], held[1, 1] = joined(found)
    now = []
    for flip, cross in ways:
        k = 2 * flip + cross
        now.append(copy(held.at[1], slots.at[2, k], base + 16 + k, device(2, flip, cross)))
    for made in now:
        made.wait_recv()
    found = [(held[1, 0], held[1, 1])]
    found += [(slots[2, 2 * flip, 0], slots[2, 2 * flip, 1]) for flip in (1, 2, 3)]
    own = joined(found)
    other = joined([(slots[2, 2 * flip + 1, 0], slots[2, 2 * flip + 1, 1]) for flip in range(4)])
    return own, other, started


def target_kernel(
    pieces, total_noise, data_ref, noise_ref, target_ref, data, data_hi, data_lo, anchor, anchor_hi,
    anchor_lo, score, running, pairs, held, slots, local_sem, send_sem, recv_sem,
):
    place = Place()
    f32, bf16 = jnp.float32, jnp.bfloat16
    rows = data.shape[4]
    share, width = anchor.shape
    chunks, _, chunk = score.shape
    total_data = chunks * chunk
    start = pl.multiple_of(place.row * rows, rows)
    unit = data.at[(place.core, *place.q)]
    bring = pltpu.make_async_copy(data_ref.at[pl.ds(start, rows)], unit, local_sem.at[0])
    bring.start()
    first = pl.multiple_of(place.col * share, share)
    noise = pltpu.make_async_copy(noise_ref.at[pl.ds(first, share)], anchor, local_sem.at[1])
    noise.start()
    meet_all(place)
    bring.wait()
    noise.wait()
    x = anchor[...]
    high = x.astype(bf16)
    anchor_hi[...] = high
    anchor_lo[...] = (x - high.astype(f32)).astype(bf16)
    noise_sq = jnp.sum(x * x, axis=1, keepdims=True)
    gather_phases(place, data, pieces, (send_sem, recv_sem), 0)

    across = (((1,), (1,)), ((), ()))
    lanes = 128
    tiles = chunk // lanes
    running[...] = jnp.full_like(running, -jnp.inf)

    @pl.loop(0, chunks)
    def _(i):
        points = data[i // 8, (i // 2) % 4, pl.ds((i % 2) * 2, 2)].reshape(chunk, width)
        high = points.astype(bf16)
        low = (points - high.astype(f32)).astype(bf16)
        data_hi[i] = high
        data_lo[i] = low
        square = points * points
        part = square[:, :lanes]
        for k in range(1, width // lanes):
            part = part + square[:, k * lanes : (k + 1) * lanes]
        data_sq = jnp.sum(part.T, axis=0, keepdims=True)
        inner = lax.dot_general(anchor_hi[...], high, across, preferred_element_type=f32)
        inner += lax.dot_general(anchor_hi[...], low, across, preferred_element_type=f32)
        inner += lax.dot_general(anchor_lo[...], high, across, preferred_element_type=f32)
        cost = (noise_sq + data_sq - 2.0 * inner) * (1.0 / width)
        found = cost * (-1.0 / ENTROPY)
        score[i] = found
        peak = running[...]
        for k in range(tiles):
            peak = jnp.maximum(peak, found[:, k * lanes : (k + 1) * lanes])
        running[...] = peak

    peak = jnp.max(running[...], axis=1, keepdims=True)
    running[...] = jnp.zeros_like(running)

    @pl.loop(0, chunks)
    def _(i):
        e = jnp.exp(score[i] - peak)
        total = running[...]
        for k in range(tiles):
            total = total + e[:, k * lanes : (k + 1) * lanes]
        running[...] = total

    total = jnp.sum(running[...], axis=1, keepdims=True)
    row_lse = peak + jnp.log(total) - math.log(float(total_data))

    @pl.loop(0, chunks)
    def _(i):
        s = score[i] - row_lse
        col_peak = jnp.max(s, axis=0, keepdims=True)
        col_total = jnp.sum(jnp.exp(s - col_peak), axis=0, keepdims=True)
        for k in range(tiles):
            at = i * tiles + k
            cols = slice(k * lanes, (k + 1) * lanes)
            pairs[at // 16, 0, pl.ds(at % 16, 1), :] = col_peak[:, cols]
            pairs[at // 16, 1, pl.ds(at % 16, 1), :] = col_total[:, cols]

    base = GATHERS * len(pieces)
    own, other, started = join_columns(place, pairs, held, slots, send_sem, recv_sem, base)
    for made in started:
        made.wait_send()
    log_noise = math.log(float(total_noise))
    pairs[place.core, 0] = own[0] + jnp.log(own[1]) - log_noise
    pairs[1 - place.core, 0] = other[0] + jnp.log(other[1]) - log_noise
    running[...] = jnp.full_like(running, -jnp.inf)

    @pl.loop(0, chunks)
    def _(i):
        peak = running[...]
        for k in range(tiles):
            at = i * tiles + k
            cols = slice(k * lanes, (k + 1) * lanes)
            s = score[i, :, cols] - pairs[at // 16, 0, pl.ds(at % 16, 1), :]
            score[i, :, cols] = s
            peak = jnp.maximum(peak, s)
        running[...] = peak

    peak = jnp.max(running[...], axis=1, keepdims=True)
    running[...] = jnp.zeros_like(running)
    target_ref[...] = jnp.zeros_like(target_ref)

    @pl.loop(0, chunks)
    def _(i):
        weights = jnp.exp(score[i] - peak).astype(bf16)
        total = running[...]
        for k in range(tiles):
            total = total + weights[:, k * lanes : (k + 1) * lanes].astype(f32)
        running[...] = total
        target_ref[...] += jnp.dot(
            weights, data_hi[i], preferred_element_type=f32
        ) + jnp.dot(weights, data_lo[i], preferred_element_type=f32)

    target_ref[...] = target_ref[...] / jnp.sum(running[...], axis=1, keepdims=True)


def find_target(noise_points, data_points, total_noise, share):
    count, width = data_points.shape
    peers = lax.axis_size("row")
    rows = count // peers
    total_data = count * lax.axis_size("col")
    quarter, tile = rows // 4, width // 4
    every = slice(None)
    last = slice(3 * quarter, rows)
    pieces = (
        (slice(0, quarter), every, 0),
        (slice(quarter, 2 * quarter), every, 1),
        (slice(2 * quarter, 3 * quarter), every, 2),
        (last, slice(0, tile), 0),
        (last, slice(tile, 2 * tile), 1),
        (last, slice(2 * tile, width), 2),
    )
    copies = GATHERS * len(pieces) + 24
    chunk = 8 * rows
    chunks = total_data // chunk
    f32, bf16 = jnp.float32, jnp.bfloat16
    half = (2, total_data // 256, 128)
    return pl.pallas_call(
        functools.partial(target_kernel, pieces, total_noise),
        out_shape=jax.ShapeDtypeStruct((share, width), f32),
        in_specs=[pl.BlockSpec(memory_space=pl.ANY)] * 2,
        out_specs=pl.BlockSpec(memory_space=pltpu.VMEM),
        scratch_shapes=[
            pltpu.VMEM((2, 4, 4, 4, rows, width), f32),
            pltpu.VMEM((chunks, chunk, width), bf16),
            pltpu.VMEM((chunks, chunk, width), bf16),
            pltpu.VMEM((share, width), f32),
            pltpu.VMEM((share, width), bf16),
            pltpu.VMEM((share, width), bf16),
            pltpu.VMEM((chunks, share, chunk), f32),
            pltpu.VMEM((share, 128), f32),
            pltpu.VMEM((2, *half), f32),
            pltpu.VMEM((2, *half), f32),
            pltpu.VMEM((3, 8, *half), f32),
            pltpu.SemaphoreType.DMA((2,)),
            pltpu.SemaphoreType.DMA((copies,)),
            pltpu.SemaphoreType.DMA((copies,)),
        ],
        compiler_params=pltpu.CompilerParams(
            collective_id=1, has_side_effects=True, vmem_limit_bytes=VMEM_CAP
        ),
        name="find_target",
    )(data_points, noise_points)


def grads_kernel(
    pieces, in_ref, out_ref, acc, from_core, slot_0, slot_1, slot_2, send_sem, recv_sem
):
    place = Place()
    core = place.core
    meet(place)
    count = len(pieces)

    def copy(src, dst, number, device):
        made = pltpu.make_async_remote_copy(
            src_ref=src, dst_ref=dst, send_sem=send_sem.at[number], recv_sem=recv_sem.at[number],
            device_id=device, device_id_type=MESH,
        )
        made.start()
        started.append(made)
        return made

    every = slice(None)
    other = 1 - core
    started = []
    first = []
    for n, (_, cols, turn) in enumerate(pieces):
        first.append(copy(in_ref.at[other, :, :, :, :, cols], from_core.at[:, :, :, :, cols], n,
                          place.other_core()))
    base = count
    halves = (pl.ds(0, 2), pl.ds(2, 2))
    landed = []

    def part(turn, flip, half, cols):
        lead = at_groups(turn, place.flipped(turn, flip), halves[half])
        return (*lead, every, cols)

    for n, (_, cols, turn) in enumerate(pieces):
        first[n].wait_recv()
        wide = slice(0, cols.stop - cols.start)

        @pl.loop(0, 16)
        def _(i, cols=cols):
            a, b = i // 4, i % 4
            acc[a, b, :, :, cols] = in_ref[core, a, b, :, :, cols] + from_core[a, b, :, :, cols]

        now = {}
        for flip, half, kind in ((3, 0, 0), (3, 1, 0), (1, 0, 1), (2, 1, 1)):
            way = 1 + half if kind == 0 else flip
            number = base + n * 6 + 2 * kind + (way - 1)
            dst = slot_0.at[n, 2 * kind + way - 1]
            now[kind, way] = copy(
                acc.at[part(turn, flip, half, cols)],
                view(dst, turn, wide), number, place.partner(turn, way),
            )
        landed.append(now)
    for way, half in ((1, 0), (2, 1)):
        for n, (_, cols, turn) in enumerate(pieces):
            wide = slice(0, cols.stop - cols.start)
            landed[n][0, way].wait_recv()
            spot = part(turn, 3 - way, half, cols)
            acc[spot] = acc[spot] + view(slot_0.at[n, way - 1], turn, wide)[...]
            number = base + n * 6 + 4 + (2 - way)
            landed[n][2, 3 - way] = copy(
                acc.at[spot], view(slot_0.at[n, 4 + 2 - way], turn, wide), number,
                place.partner(turn, 3 - way),
            )
    base += 6 * count
    for n, (_, cols, turn) in enumerate(pieces):
        wide = slice(0, cols.stop - cols.start)
        for kind in (1, 2):
            for way in (1, 2):
                landed[n][kind, way].wait_recv()
        for half in (0, 1):
            spot = part(turn, 0, half, cols)
            one, two = (2, 5) if half == 0 else (3, 4)
            acc[spot] = acc[spot] + (
                view(slot_0.at[n, one], turn, wide)[...] + view(slot_0.at[n, two], turn, wide)[...]
            )
    waiting = [[] for _ in pieces]
    for n, (_, cols, turn) in enumerate(pieces):
        wide = slice(0, cols.stop - cols.start)
        group = (turn + 1) % 3
        for flip in (1, 2, 3):
            src = acc.at[(*at_groups(turn, place.q[turn], place.flipped(group, flip)), every, cols)]
            waiting[n].append(
                copy(src, slot_1.at[n, flip - 1, :, :, wide], base + n * 3 + flip - 1,
                     place.partner(group, flip))
            )
    base += 3 * count
    for n, (_, cols, turn) in enumerate(pieces):
        wide = slice(0, cols.stop - cols.start)
        for made in waiting[n]:
            made.wait_recv()
        waiting[n] = []
        group = (turn + 2) % 3
        spot = (*at_groups(turn, place.q[turn], place.q[(turn + 1) % 3]), every, cols)
        acc[spot] = (acc[spot] + slot_1[n, 0, :, :, wide]) + (
            slot_1[n, 1, :, :, wide] + slot_1[n, 2, :, :, wide]
        )
        for flip in (1, 2, 3):
            waiting[n].append(
                copy(acc.at[spot], slot_2.at[n, flip - 1, :, :, wide], base + n * 3 + flip - 1,
                     place.partner(group, flip))
            )
    base += 3 * count
    for n, (_, cols, turn) in enumerate(pieces):
        wide = slice(0, cols.stop - cols.start)
        for made in waiting[n]:
            made.wait_recv()
        spot = (*at_groups(turn, place.q[turn], place.q[(turn + 1) % 3]), every, cols)
        out_ref[(core, *spot)] = (acc[spot] + slot_2[n, 0, :, :, wide]) + (
            slot_2[n, 1, :, :, wide] + slot_2[n, 2, :, :, wide]
        )
    gather_phases(place, out_ref, pieces, (send_sem, recv_sem), base, (1, 2))
    for made in started:
        made.wait_send()


def view(ref, turn, wide):
    shape = [None, None]
    where = [(turn + 1) % 3, (turn + 2) % 3]
    shape = (2, 4) if where[0] < where[1] else (4, 2)
    return ref.reshape(*shape, *ref.shape[1:]).at[:, :, :, wide]


def sum_grads(grads):
    shape = grads.shape
    width = shape[-1]
    share = 128 * -(-width // 384)
    every = slice(None)
    pieces = (
        (every, slice(0, share), 0),
        (every, slice(share, 2 * share), 1),
        (every, slice(2 * share, width), 2),
    )
    copies = (1 + 6 + 6 + GATHERS) * len(pieces)
    f32 = jnp.float32
    return pl.pallas_call(
        functools.partial(grads_kernel, pieces),
        out_shape=jax.ShapeDtypeStruct(shape, f32),
        in_specs=[pl.BlockSpec(memory_space=pltpu.VMEM)],
        out_specs=pl.BlockSpec(memory_space=pltpu.VMEM),
        scratch_shapes=[
            pltpu.VMEM(shape[1:], f32),
            pltpu.VMEM(shape[1:], f32),
            pltpu.VMEM((3, 6, 8, 8, share), f32),
            pltpu.VMEM((3, 3, 4, 8, share), f32),
            pltpu.VMEM((3, 3, 4, 8, share), f32),
            pltpu.SemaphoreType.DMA((copies,)),
            pltpu.SemaphoreType.DMA((copies,)),
        ],
        compiler_params=pltpu.CompilerParams(
            collective_id=3, has_side_effects=True, vmem_limit_bytes=VMEM_CAP
        ),
        name="sum_grads",
    )(grads)


def spread(rows, steps_each):
    count, width = rows.shape
    wide = jnp.broadcast_to(rows[:, None, :], (count, steps_each, width))
    return wide.reshape(count * steps_each, width)


def train_kernel(
    scale, points, steps_each, anchor_ref, target_ref, tvals_ref, shift_ref, w_in_ref, w_out_ref,
    w_back_ref, predicted_ref, grads_ref, mixed_ref, hidden_ref, delta_ref, delta_pre_ref,
):
    block = points * steps_each
    width, hid_width = w_in_ref.shape
    blocks = anchor_ref.shape[0] // points
    grads_ref[...] = jnp.zeros_like(grads_ref)
    f32, bf16 = jnp.float32, jnp.bfloat16
    contract = (((0,), (0,)), ((), ()))
    lanes = 128

    def forward(b, slot):
        here = pl.ds(pl.multiple_of(b * points, points), points)
        anchor, target = anchor_ref[here, :], target_ref[here, :]
        tvals = tvals_ref[pl.ds(pl.multiple_of(b * block, block), block), :]
        parts = []
        for k in range(width // lanes):
            cols = slice(k * lanes, (k + 1) * lanes)
            x, y = spread(anchor[:, cols], steps_each), spread(target[:, cols], steps_each)
            parts.append(((1.0 - tvals) * x + tvals * y).astype(bf16))
        mixed = jnp.concatenate(parts, axis=1)
        mixed_ref[slot] = mixed
        pre = jnp.dot(mixed, w_in_ref[...], preferred_element_type=f32)
        shift = jnp.concatenate(
            [tvals * shift_ref[:, k * lanes : (k + 1) * lanes] for k in range(hid_width // lanes)],
            axis=1,
        )
        pre = pre + shift
        sig = 0.5 * jnp.tanh(0.5 * pre) + 0.5
        hidden = (pre * sig).astype(bf16)
        slope = sig * (1.0 + pre * (1.0 - sig))
        hidden_ref[slot] = hidden
        output = jnp.dot(hidden, w_out_ref[...], preferred_element_type=f32)
        predicted_ref[pl.ds(pl.multiple_of(b * block, block), block), :] = output.astype(bf16)
        velocity = spread(target - anchor, steps_each)
        delta = ((output - velocity) * scale).astype(bf16)
        delta_ref[slot] = delta
        back = jnp.dot(delta, w_back_ref[...], preferred_element_type=f32)
        delta_pre_ref[slot] = (back * slope).astype(bf16)

    def add_grads(slot):
        grads_ref[0] += lax.dot_general(
            mixed_ref[slot], delta_pre_ref[slot], contract, preferred_element_type=f32
        )
        for k in range(hid_width // width):
            cols = slice(k * width, (k + 1) * width)
            grads_ref[1, :, cols] += lax.dot_general(
                hidden_ref[slot, :, cols], delta_ref[slot], contract, preferred_element_type=f32
            )

    forward(0, 0)

    @pl.loop(1, blocks)
    def _(b):
        forward(b, b % 2)
        add_grads((b + 1) % 2)

    add_grads((blocks - 1) % 2)


def train(anchor, target, times, time_shift, weight_in, weight_out, scale):
    share, width = anchor.shape
    hid_width = weight_in.shape[1]
    steps_each = times.shape[1]
    points = 32
    block = points * steps_each
    tvals = jnp.broadcast_to(times.reshape(share * steps_each, 1), (share * steps_each, 128))
    bf16 = jnp.bfloat16
    vmem = pl.BlockSpec(memory_space=pltpu.VMEM)
    return pl.pallas_call(
        functools.partial(train_kernel, scale, points, steps_each),
        out_shape=(
            jax.ShapeDtypeStruct((share * steps_each, width), bf16),
            jax.ShapeDtypeStruct((2, width, hid_width), jnp.float32),
        ),
        in_specs=[vmem] * 7,
        out_specs=(vmem, vmem),
        scratch_shapes=[
            pltpu.VMEM((2, block, width), bf16),
            pltpu.VMEM((2, block, hid_width), bf16),
            pltpu.VMEM((2, block, width), bf16),
            pltpu.VMEM((2, block, hid_width), bf16),
        ],
        compiler_params=pltpu.CompilerParams(vmem_limit_bytes=VMEM_CAP),
        name="train",
    )(anchor, target, tvals, time_shift.reshape(1, hid_width), weight_in, weight_out, weight_out.T)


def on_device(noise_points, data_points, times, time_shift, weight_in, weight_out):
    count_row = lax.axis_size("row")
    count_col = lax.axis_size("col")
    rows_here = noise_points.shape[0]
    total_noise = rows_here * count_row
    width = noise_points.shape[1]
    share = rows_here // count_col
    steps_each = times.shape[1]

    target = find_target(noise_points, data_points, total_noise, share)
    anchor = lax.dynamic_slice_in_dim(noise_points, lax.axis_index("col") * share, share, 0)
    scale = 1.0 / math.sqrt(float(total_noise * steps_each))
    predicted, grads = train(
        anchor, target, times, time_shift, weight_in, weight_out, scale
    )
    hid_width = weight_in.shape[1]
    halves = hid_width // width
    grads = grads.reshape(2, 4, 4, 4, width // 64, hid_width)
    summed = sum_grads(grads).reshape(2, width, hid_width)
    grad_in = summed[0]
    grad_out = jnp.concatenate(
        [summed[1][:, k * width : (k + 1) * width] for k in range(halves)], axis=0
    )
    return (predicted, grad_in, grad_out)


def solution(mesh):
    in_specs = (P("row", None), P("col", None), P(("row", "col"), None), P(), P(), P())
    out_specs = (P(("row", "col"), None), P(), P())
    return jax.shard_map(
        on_device, mesh=mesh, in_specs=in_specs, out_specs=out_specs, check_vma=False
    )
```

```python
import functools
import math

import jax
import jax.numpy as jnp
from jax import lax
from jax.experimental import pallas as pl
from jax.experimental.pallas import tpu as pltpu
from jax.sharding import PartitionSpec as P

ENTROPY = 0.05
MESH = pl.DeviceIdType.MESH
VMEM_CAP = 54 * 1024 * 1024
GATHERS = 19


class Place:
    def __init__(self):
        row, col = lax.axis_index("row"), lax.axis_index("col")
        self.core = col % 2
        x = (row % 2) * 2 + (col // 2) % 2
        y = row // 2
        z = col // 4
        self.bits = []
        for pos in (x, y, z):
            self.bits.append(((pos + pos // 2) % 2, pos // 2))
        (xa, xb), (ya, yb), (za, zb) = self.bits
        self.groups = ((xa, ya), (yb, za), (zb, xb))
        self.q = tuple(u * 2 + v for u, v in self.groups)
        self.row, self.col = row, col

    def partner(self, group, flip, cross=0):
        hi, lo = flip // 2, flip % 2
        core = 1 - self.core if cross else self.core
        groups = [list(g) for g in self.groups]
        if hi:
            groups[group][0] = 1 - groups[group][0]
        if lo:
            groups[group][1] = 1 - groups[group][1]
        (xa, ya), (yb, za), (zb, xb) = groups
        x, y, z = ((2 * b + (a + b) % 2) for a, b in ((xa, xb), (ya, yb), (za, zb)))
        return (y * 2 + x // 2, z * 4 + (x % 2) * 2 + core)

    def other_core(self):
        return (self.row, self.col + 1 - 2 * self.core)

    def flipped(self, group, flip):
        hi, lo = self.groups[group]
        if flip // 2:
            hi = 1 - hi
        if flip % 2:
            lo = 1 - lo
        return hi * 2 + lo


def at_groups(turn, first=None, second=None, third=None):
    found = [slice(None)] * 3
    for k, value in enumerate((first, second, third)):
        if value is not None:
            found[(turn + k) % 3] = value
    return tuple(found)


def gather_phases(place, out, pieces, sems, base, phases=(0, 1, 2)):
    send, recv = sems
    mine = out.at[place.core]
    started = []

    def copy(block, number, device):
        made = pltpu.make_async_remote_copy(
            src_ref=block, dst_ref=block, send_sem=send.at[number], recv_sem=recv.at[number],
            device_id=device, device_id_type=MESH,
        )
        made.start()
        started.append(made)
        return made

    def spot(piece, *values):
        rows, cols, turn = piece
        return mine.at[(*at_groups(turn, *values), rows, cols)]

    waiting = [[] for _ in pieces]
    for phase in phases[:-1]:
        for n, piece in enumerate(pieces):
            turn = piece[2]
            q = [place.q[(turn + k) % 3] for k in range(3)]
            for made in waiting[n]:
                made.wait_recv()
            waiting[n] = []
            group = (turn + 2 - phase) % 3
            block = spot(piece, *(q, q[:2])[phase])
            for flip in (1, 2, 3):
                number = base + GATHERS * n + phase * 3 + flip - 1
                waiting[n].append(copy(block, number, place.partner(group, flip)))
    halves = (pl.ds(0, 2), pl.ds(2, 2))
    across, landed = [], []
    for n, piece in enumerate(pieces):
        turn = piece[2]
        for made in waiting[n]:
            made.wait_recv()
        first = base + GATHERS * n + 6
        own = place.q[turn]
        now = {}
        for k in range(2):
            for flip, half in ((2, k), (1, 1 - k)):
                block = spot(piece, own, halves[half])
                now[flip, half] = copy(block, first + 2 * (flip - 1) + half,
                                       place.partner(turn, flip))
        across.append(copy(spot(piece, own), first + 6, place.other_core()))
        landed.append(now)
    for flip, half, step in ((2, 0, 0), (1, 1, 0), (2, 1, 1), (1, 0, 1)):
        for n, piece in enumerate(pieces):
            turn = piece[2]
            first = base + GATHERS * n + 6
            landed[n][flip, half].wait_recv()
            block = spot(piece, place.flipped(turn, flip), halves[half])
            if step == 0:
                landed[n][3, half] = copy(block, first + 4 + half, place.partner(turn, 3 - flip))
            across.append(
                copy(block, first + 7 + 2 * (flip - 1) + half, place.other_core())
            )
    for half in range(2):
        for n, piece in enumerate(pieces):
            turn = piece[2]
            first = base + GATHERS * n + 6
            landed[n][3, half].wait_recv()
            block = spot(piece, place.flipped(turn, 3), halves[half])
            across.append(copy(block, first + 11 + half, place.other_core()))
    for made in across:
        made.wait_recv()
    for made in started:
        made.wait_send()


def greet(place):
    barrier = pltpu.get_barrier_semaphore()
    known = [place.other_core()]
    for group, both in ((0, True), (1, False), (2, True)):
        for flip in (1, 2, 3):
            known.append(place.partner(group, flip))
            if both:
                known.append(place.partner(group, flip, 1))
    for device in known:
        pl.semaphore_signal(barrier, inc=1, device_id=device, device_id_type=MESH)
    return len(known)


def joined(pairs):
    peak = pairs[0][0]
    for other, _ in pairs[1:]:
        peak = jnp.maximum(peak, other)
    total = pairs[0][1] * jnp.exp(pairs[0][0] - peak)
    for other, amount in pairs[1:]:
        total = total + amount * jnp.exp(other - peak)
    return peak, total


def join_columns(place, pairs, held, slots, send, recv, base):
    core = place.core
    started = []

    def copy(src, dst, number, device):
        made = pltpu.make_async_remote_copy(
            src_ref=src, dst_ref=dst, send_sem=send.at[number], recv_sem=recv.at[number],
            device_id=device, device_id_type=MESH,
        )
        made.start()
        started.append(made)
        return made

    def device(group, flip, cross):
        return place.other_core() if flip == 0 else place.partner(group, flip, cross)

    ways = [(flip, cross) for flip in range(4) for cross in range(2) if flip or cross]
    now = []
    for flip, cross in ways:
        k = 2 * flip + cross
        half = 1 - core if cross else core
        now.append(copy(pairs.at[half], slots.at[0, k], base + k, device(0, flip, cross)))
    for made in now:
        made.wait_recv()
    found = [(pairs[core, 0], pairs[core, 1])]
    found += [(slots[0, 2 * f + c, 0], slots[0, 2 * f + c, 1]) for f, c in ways]
    held[0, 0], held[0, 1] = joined(found)
    now = []
    for flip in (1, 2, 3):
        number = base + 8 + flip
        now.append(copy(held.at[0], slots.at[1, flip], number, device(1, flip, 0)))
    for made in now:
        made.wait_recv()
    found = [(held[0, 0], held[0, 1])]
    found += [(slots[1, flip, 0], slots[1, flip, 1]) for flip in (1, 2, 3)]
    held[1, 0], held[1, 1] = joined(found)
    now = []
    for flip, cross in ways:
        k = 2 * flip + cross
        now.append(copy(held.at[1], slots.at[2, k], base + 16 + k, device(2, flip, cross)))
    for made in now:
        made.wait_recv()
    found = [(held[1, 0], held[1, 1])]
    found += [(slots[2, 2 * flip, 0], slots[2, 2 * flip, 1]) for flip in (1, 2, 3)]
    own = joined(found)
    other = joined([(slots[2, 2 * flip + 1, 0], slots[2, 2 * flip + 1, 1]) for flip in range(4)])
    return own, other, started


def find_target(
    place, pieces, total_noise, target_ref, data, data_hi, data_lo, anchor, anchor_hi, anchor_lo,
    score, running, pairs, held, slots, send_sem, recv_sem,
):
    f32, bf16 = jnp.float32, jnp.bfloat16
    width = anchor.shape[1]
    chunks, _, chunk = score.shape
    total_data = chunks * chunk
    gather_phases(place, data, pieces, (send_sem, recv_sem), 0)
    x = anchor[...]
    noise_sq = jnp.sum(x * x, axis=1, keepdims=True)

    across = (((1,), (1,)), ((), ()))
    lanes = 128
    tiles = chunk // lanes
    running[...] = jnp.full_like(running, -jnp.inf)

    @pl.loop(0, chunks)
    def _(i):
        points = data[i // 8, (i // 2) % 4, pl.ds((i % 2) * 2, 2)].reshape(chunk, width)
        high = points.astype(bf16)
        low = (points - high.astype(f32)).astype(bf16)
        data_hi[i] = high
        data_lo[i] = low
        square = points * points
        part = square[:, :lanes]
        for k in range(1, width // lanes):
            part = part + square[:, k * lanes : (k + 1) * lanes]
        data_sq = jnp.sum(part.T, axis=0, keepdims=True)
        inner = lax.dot_general(anchor_hi[...], high, across, preferred_element_type=f32)
        inner += lax.dot_general(anchor_hi[...], low, across, preferred_element_type=f32)
        inner += lax.dot_general(anchor_lo[...], high, across, preferred_element_type=f32)
        cost = (noise_sq + data_sq - 2.0 * inner) * (1.0 / width)
        found = cost * (-1.0 / ENTROPY)
        score[i] = found
        peak = running[...]
        for k in range(tiles):
            peak = jnp.maximum(peak, found[:, k * lanes : (k + 1) * lanes])
        running[...] = peak

    peak = jnp.max(running[...], axis=1, keepdims=True)
    running[...] = jnp.zeros_like(running)

    @pl.loop(0, chunks)
    def _(i):
        e = jnp.exp(score[i] - peak)
        total = running[...]
        for k in range(tiles):
            total = total + e[:, k * lanes : (k + 1) * lanes]
        running[...] = total

    total = jnp.sum(running[...], axis=1, keepdims=True)
    row_lse = peak + jnp.log(total) - math.log(float(total_data))

    @pl.loop(0, chunks)
    def _(i):
        s = score[i] - row_lse
        col_peak = jnp.max(s, axis=0, keepdims=True)
        col_total = jnp.sum(jnp.exp(s - col_peak), axis=0, keepdims=True)
        for k in range(tiles):
            at = i * tiles + k
            cols = slice(k * lanes, (k + 1) * lanes)
            pairs[at // 16, 0, pl.ds(at % 16, 1), :] = col_peak[:, cols]
            pairs[at // 16, 1, pl.ds(at % 16, 1), :] = col_total[:, cols]

    base = GATHERS * len(pieces)
    own, other, started = join_columns(place, pairs, held, slots, send_sem, recv_sem, base)
    for made in started:
        made.wait_send()
    log_noise = math.log(float(total_noise))
    pairs[place.core, 0] = own[0] + jnp.log(own[1]) - log_noise
    pairs[1 - place.core, 0] = other[0] + jnp.log(other[1]) - log_noise
    running[...] = jnp.full_like(running, -jnp.inf)

    @pl.loop(0, chunks)
    def _(i):
        peak = running[...]
        for k in range(tiles):
            at = i * tiles + k
            cols = slice(k * lanes, (k + 1) * lanes)
            s = score[i, :, cols] - pairs[at // 16, 0, pl.ds(at % 16, 1), :]
            score[i, :, cols] = s
            peak = jnp.maximum(peak, s)
        running[...] = peak

    peak = jnp.max(running[...], axis=1, keepdims=True)
    running[...] = jnp.zeros_like(running)
    target_ref[...] = jnp.zeros_like(target_ref)

    @pl.loop(0, chunks)
    def _(i):
        weights = jnp.exp(score[i] - peak).astype(bf16)
        total = running[...]
        for k in range(tiles):
            total = total + weights[:, k * lanes : (k + 1) * lanes].astype(f32)
        running[...] = total
        target_ref[...] += jnp.dot(
            weights, data_hi[i], preferred_element_type=f32
        ) + jnp.dot(weights, data_lo[i], preferred_element_type=f32)

    target_ref[...] = target_ref[...] / jnp.sum(running[...], axis=1, keepdims=True)


def sum_grads(
    place, pieces, in_ref, out_ref, acc, from_core, slot_0, slot_1, slot_2, send_sem, recv_sem
):
    core = place.core
    count = len(pieces)

    def copy(src, dst, number, device):
        made = pltpu.make_async_remote_copy(
            src_ref=src, dst_ref=dst, send_sem=send_sem.at[number], recv_sem=recv_sem.at[number],
            device_id=device, device_id_type=MESH,
        )
        made.start()
        started.append(made)
        return made

    every = slice(None)
    other = 1 - core
    started = []
    first = []
    for n, (_, cols, turn) in enumerate(pieces):
        first.append(copy(in_ref.at[other, :, :, :, :, cols], from_core.at[:, :, :, :, cols], n,
                          place.other_core()))
    base = count
    halves = (pl.ds(0, 2), pl.ds(2, 2))
    landed = []

    def part(turn, flip, half, cols):
        lead = at_groups(turn, place.flipped(turn, flip), halves[half])
        return (*lead, every, cols)

    for n, (_, cols, turn) in enumerate(pieces):
        first[n].wait_recv()
        wide = slice(0, cols.stop - cols.start)

        @pl.loop(0, 16)
        def _(i, cols=cols):
            a, b = i // 4, i % 4
            acc[a, b, :, :, cols] = in_ref[core, a, b, :, :, cols] + from_core[a, b, :, :, cols]

        now = {}
        for flip, half, kind in ((3, 0, 0), (3, 1, 0), (1, 0, 1), (2, 1, 1)):
            way = 1 + half if kind == 0 else flip
            number = base + n * 6 + 2 * kind + (way - 1)
            dst = slot_0.at[n, 2 * kind + way - 1]
            now[kind, way] = copy(
                acc.at[part(turn, flip, half, cols)],
                view(dst, turn, wide), number, place.partner(turn, way),
            )
        landed.append(now)
    for way, half in ((1, 0), (2, 1)):
        for n, (_, cols, turn) in enumerate(pieces):
            wide = slice(0, cols.stop - cols.start)
            landed[n][0, way].wait_recv()
            spot = part(turn, 3 - way, half, cols)
            acc[spot] = acc[spot] + view(slot_0.at[n, way - 1], turn, wide)[...]
            number = base + n * 6 + 4 + (2 - way)
            landed[n][2, 3 - way] = copy(
                acc.at[spot], view(slot_0.at[n, 4 + 2 - way], turn, wide), number,
                place.partner(turn, 3 - way),
            )
    base += 6 * count
    for n, (_, cols, turn) in enumerate(pieces):
        wide = slice(0, cols.stop - cols.start)
        for kind in (1, 2):
            for way in (1, 2):
                landed[n][kind, way].wait_recv()
        for half in (0, 1):
            spot = part(turn, 0, half, cols)
            one, two = (2, 5) if half == 0 else (3, 4)
            acc[spot] = acc[spot] + (
                view(slot_0.at[n, one], turn, wide)[...] + view(slot_0.at[n, two], turn, wide)[...]
            )
    waiting = [[] for _ in pieces]
    for n, (_, cols, turn) in enumerate(pieces):
        wide = slice(0, cols.stop - cols.start)
        group = (turn + 1) % 3
        for flip in (1, 2, 3):
            src = acc.at[(*at_groups(turn, place.q[turn], place.flipped(group, flip)), every, cols)]
            waiting[n].append(
                copy(src, slot_1.at[n, flip - 1, :, :, wide], base + n * 3 + flip - 1,
                     place.partner(group, flip))
            )
    base += 3 * count
    for n, (_, cols, turn) in enumerate(pieces):
        wide = slice(0, cols.stop - cols.start)
        for made in waiting[n]:
            made.wait_recv()
        waiting[n] = []
        group = (turn + 2) % 3
        spot = (*at_groups(turn, place.q[turn], place.q[(turn + 1) % 3]), every, cols)
        acc[spot] = (acc[spot] + slot_1[n, 0, :, :, wide]) + (
            slot_1[n, 1, :, :, wide] + slot_1[n, 2, :, :, wide]
        )
        for flip in (1, 2, 3):
            waiting[n].append(
                copy(acc.at[spot], slot_2.at[n, flip - 1, :, :, wide], base + n * 3 + flip - 1,
                     place.partner(group, flip))
            )
    base += 3 * count
    for n, (_, cols, turn) in enumerate(pieces):
        wide = slice(0, cols.stop - cols.start)
        for made in waiting[n]:
            made.wait_recv()
        spot = (*at_groups(turn, place.q[turn], place.q[(turn + 1) % 3]), every, cols)
        out_ref[(core, *spot)] = (acc[spot] + slot_2[n, 0, :, :, wide]) + (
            slot_2[n, 1, :, :, wide] + slot_2[n, 2, :, :, wide]
        )
    gather_phases(place, out_ref, pieces, (send_sem, recv_sem), base, (1, 2))
    for made in started:
        made.wait_send()


def view(ref, turn, wide):
    shape = [None, None]
    where = [(turn + 1) % 3, (turn + 2) % 3]
    shape = (2, 4) if where[0] < where[1] else (4, 2)
    return ref.reshape(*shape, *ref.shape[1:]).at[:, :, :, wide]


def spread(rows, steps_each):
    count, width = rows.shape
    wide = jnp.broadcast_to(rows[:, None, :], (count, steps_each, width))
    return wide.reshape(count * steps_each, width)


def train(
    scale, points, steps_each, anchor_ref, target_ref, tvals_ref, shift_ref, w_in_ref, w_out_ref,
    w_back_ref, predicted_ref, grads_ref, mixed_ref, hidden_ref, delta_ref, delta_pre_ref,
):
    block = points * steps_each
    width, hid_width = w_in_ref.shape
    blocks = anchor_ref.shape[0] // points
    f32, bf16 = jnp.float32, jnp.bfloat16
    contract = (((0,), (0,)), ((), ()))
    lanes = 128

    def forward(b, slot):
        here = pl.ds(pl.multiple_of(b * points, points), points)
        anchor, target = anchor_ref[here, :], target_ref[here, :]
        tvals = tvals_ref[pl.ds(pl.multiple_of(b * block, block), block), :]
        parts = []
        for k in range(width // lanes):
            cols = slice(k * lanes, (k + 1) * lanes)
            x, y = spread(anchor[:, cols], steps_each), spread(target[:, cols], steps_each)
            parts.append(((1.0 - tvals) * x + tvals * y).astype(bf16))
        mixed = jnp.concatenate(parts, axis=1)
        mixed_ref[slot] = mixed
        pre = jnp.dot(mixed, w_in_ref[...], preferred_element_type=f32)
        shift = jnp.concatenate(
            [tvals * shift_ref[:, k * lanes : (k + 1) * lanes] for k in range(hid_width // lanes)],
            axis=1,
        )
        pre = pre + shift
        sig = 0.5 * jnp.tanh(0.5 * pre) + 0.5
        hidden = (pre * sig).astype(bf16)
        slope = sig * (1.0 + pre * (1.0 - sig))
        hidden_ref[slot] = hidden
        output = jnp.dot(hidden, w_out_ref[...], preferred_element_type=f32)
        predicted_ref[pl.ds(pl.multiple_of(b * block, block), block), :] = output.astype(bf16)
        velocity = spread(target - anchor, steps_each)
        delta = ((output - velocity) * scale).astype(bf16)
        delta_ref[slot] = delta
        back = jnp.dot(delta, w_back_ref[...], preferred_element_type=f32)
        delta_pre_ref[slot] = (back * slope).astype(bf16)

    def add_grads(slot):
        grads_ref[0] += lax.dot_general(
            mixed_ref[slot], delta_pre_ref[slot], contract, preferred_element_type=f32
        )
        for k in range(hid_width // width):
            cols = slice(k * width, (k + 1) * width)
            grads_ref[1, :, cols] += lax.dot_general(
                hidden_ref[slot, :, cols], delta_ref[slot], contract, preferred_element_type=f32
            )

    forward(0, 0)

    @pl.loop(1, blocks)
    def _(b):
        forward(b, b % 2)
        add_grads((b + 1) % 2)

    add_grads((blocks - 1) % 2)


def step_kernel(
    data_pieces, grad_pieces, total_noise, points, data_ref, noise_ref, times_ref, shift_ref,
    w_in_ref, w_out_ref, predicted_ref, grad_in_ref, grad_out_ref, data, data_hi, data_lo, anchor,
    anchor_hi, anchor_lo, score, running, pairs, held, slots, target, w_in, w_out, w_back, steps,
    tvals, mixed, hidden, delta, delta_pre, grads, acc, from_core, slot_0, slot_1,
    slot_2, summed, local_sem, send_sem, recv_sem, grad_send_sem, grad_recv_sem,
):
    place = Place()
    f32, bf16 = jnp.float32, jnp.bfloat16
    rows = data.shape[4]
    share, width = anchor.shape
    hid_width = w_in.shape[1]
    steps_each = times_ref.shape[0]
    start = pl.multiple_of(place.row * rows, rows)
    first = pl.multiple_of(place.col * share, share)
    loads = [
        pltpu.make_async_copy(source, to, local_sem.at[k])
        for k, (source, to) in enumerate((
            (data_ref.at[pl.ds(start, rows)], data.at[(place.core, *place.q)]),
            (noise_ref.at[pl.ds(first, share)], anchor),
            (w_out_ref, w_out),
            (w_in_ref, w_in),
        ))
    ]
    for load in loads:
        load.start()
    count = greet(place)
    grads[...] = jnp.zeros_like(grads)
    steps[...] = times_ref[...].T
    block = points * steps_each

    @pl.loop(0, share // points)
    def _(b):
        here = pl.ds(pl.multiple_of(b * points, points), points)
        wide = spread(steps[here, :], steps_each)
        row = lax.broadcasted_iota(jnp.int32, wide.shape, 0)
        lane = lax.broadcasted_iota(jnp.int32, wide.shape, 1)
        own = jnp.where(row % steps_each == lane, wide, 0.0)
        value = jnp.sum(own, axis=1, keepdims=True)
        to = pl.ds(pl.multiple_of(b * block, block), block)
        tvals[to, :] = jnp.broadcast_to(value, (block, 128))

    for load in loads:
        load.wait()
    x = anchor[...]
    high = x.astype(bf16)
    anchor_hi[...] = high
    anchor_lo[...] = (x - high.astype(f32)).astype(bf16)
    for k in range(hid_width // 256):
        part = slice(k * 256, (k + 1) * 256)
        w_back[:, part] = w_out[part, :].T
    pl.semaphore_wait(pltpu.get_barrier_semaphore(), count)
    find_target(
        place, data_pieces, total_noise, target, data, data_hi, data_lo, anchor, anchor_hi,
        anchor_lo, score, running, pairs, held, slots, send_sem, recv_sem,
    )
    scale = 1.0 / math.sqrt(float(total_noise * steps_each))
    train(
        scale, points, steps_each, anchor, target, tvals, shift_ref, w_in, w_out, w_back,
        predicted_ref, grads, mixed, hidden, delta, delta_pre,
    )
    sum_grads(
        place, grad_pieces, grads.reshape(summed.shape), summed, acc, from_core, slot_0, slot_1,
        slot_2, grad_send_sem, grad_recv_sem,
    )

    @pl.loop(0, 16)
    def _(i):
        a, b = i // 4, i % 4
        count = 4 * summed.shape[4]
        to = pl.multiple_of(i * count, count)
        grad_in_ref[pl.ds(to, count), :] = summed[0, a, b].reshape(count, hid_width)
        for k in range(hid_width // width):
            part = slice(k * width, (k + 1) * width)
            here = pl.ds(pl.multiple_of(k * width + to, count), count)
            grad_out_ref[here, :] = summed[1, a, b, :, :, part].reshape(count, width)


def on_device(noise_points, data_points, times, time_shift, weight_in, weight_out):
    count_row = lax.axis_size("row")
    count_col = lax.axis_size("col")
    total_noise = noise_points.shape[0] * count_row
    total_data = data_points.shape[0] * count_col
    width, hid_width = weight_in.shape
    share, steps_each = times.shape
    rows = data_points.shape[0] // count_row
    chunk = 8 * rows
    chunks = total_data // chunk
    points = 32
    block = points * steps_each
    quarter, tile = rows // 4, width // 4
    every = slice(None)
    last = slice(3 * quarter, rows)
    data_pieces = (
        (slice(0, quarter), every, 0),
        (slice(quarter, 2 * quarter), every, 1),
        (slice(2 * quarter, 3 * quarter), every, 2),
        (last, slice(0, tile), 0),
        (last, slice(tile, 2 * tile), 1),
        (last, slice(2 * tile, width), 2),
    )
    third = 128 * -(-hid_width // 384)
    grad_pieces = (
        (every, slice(0, third), 0),
        (every, slice(third, 2 * third), 1),
        (every, slice(2 * third, hid_width), 2),
    )
    copies = GATHERS * len(data_pieces) + 24
    grad_copies = (1 + 6 + 6 + GATHERS) * len(grad_pieces)
    f32, bf16 = jnp.float32, jnp.bfloat16
    pair = (2, total_data // 256, 128)
    units = (4, 4, 4, width // 64, hid_width)
    far = pl.BlockSpec(memory_space=pl.ANY)
    near = pl.BlockSpec(memory_space=pltpu.VMEM)
    return pl.pallas_call(
        functools.partial(step_kernel, data_pieces, grad_pieces, total_noise, points),
        out_shape=(
            pltpu.VMEM((share * steps_each, width), bf16),
            pltpu.VMEM((width, hid_width), f32),
            pltpu.VMEM((hid_width, width), f32),
        ),
        in_specs=[far, far, near, near, far, far],
        out_specs=(near, near, near),
        scratch_shapes=[
            pltpu.VMEM((2, 4, 4, 4, rows, width), f32),
            pltpu.VMEM((chunks, chunk, width), bf16),
            pltpu.VMEM((chunks, chunk, width), bf16),
            pltpu.VMEM((share, width), f32),
            pltpu.VMEM((share, width), bf16),
            pltpu.VMEM((share, width), bf16),
            pltpu.VMEM((chunks, share, chunk), f32),
            pltpu.VMEM((share, 128), f32),
            pltpu.VMEM((2, *pair), f32),
            pltpu.VMEM((2, *pair), f32),
            pltpu.VMEM((3, 8, *pair), f32),
            pltpu.VMEM((share, width), f32),
            pltpu.VMEM((width, hid_width), bf16),
            pltpu.VMEM((hid_width, width), bf16),
            pltpu.VMEM((width, hid_width), bf16),
            pltpu.VMEM((share, steps_each), f32),
            pltpu.VMEM((share * steps_each, 128), f32),
            pltpu.VMEM((2, block, width), bf16),
            pltpu.VMEM((2, block, hid_width), bf16),
            pltpu.VMEM((2, block, width), bf16),
            pltpu.VMEM((2, block, hid_width), bf16),
            pltpu.VMEM((2, width, hid_width), f32),
            pltpu.VMEM(units, f32),
            pltpu.VMEM(units, f32),
            pltpu.VMEM((3, 6, 8, width // 64, third), f32),
            pltpu.VMEM((3, 3, 4, width // 64, third), f32),
            pltpu.VMEM((3, 3, 4, width // 64, third), f32),
            pltpu.VMEM((2, *units), f32),
            pltpu.SemaphoreType.DMA((4,)),
            pltpu.SemaphoreType.DMA((copies,)),
            pltpu.SemaphoreType.DMA((copies,)),
            pltpu.SemaphoreType.DMA((grad_copies,)),
            pltpu.SemaphoreType.DMA((grad_copies,)),
        ],
        compiler_params=pltpu.CompilerParams(
            collective_id=1, has_side_effects=True, vmem_limit_bytes=VMEM_CAP
        ),
        name="step",
    )(data_points, noise_points, times.T, time_shift.reshape(1, hid_width), weight_in, weight_out)


def solution(mesh):
    in_specs = (P("row", None), P("col", None), P(("row", "col"), None), P(), P(), P())
    out_specs = (P(("row", "col"), None), P(), P())
    return jax.shard_map(
        on_device, mesh=mesh, in_specs=in_specs, out_specs=out_specs, check_vma=False
    )
```

```python
import functools
import math

import jax
import jax.numpy as jnp
from jax import lax
from jax.experimental import pallas as pl
from jax.experimental.pallas import tpu as pltpu
from jax.sharding import PartitionSpec as P

ENTROPY = 0.05
MESH = pl.DeviceIdType.MESH
VMEM_CAP = 54 * 1024 * 1024
GATHERS = 19


class Place:
    def __init__(self):
        row, col = lax.axis_index("row"), lax.axis_index("col")
        self.core = col % 2
        x = (row % 2) * 2 + (col // 2) % 2
        y = row // 2
        z = col // 4
        self.bits = []
        for pos in (x, y, z):
            self.bits.append(((pos + pos // 2) % 2, pos // 2))
        (xa, xb), (ya, yb), (za, zb) = self.bits
        self.groups = ((xa, ya), (yb, za), (zb, xb))
        self.q = tuple(u * 2 + v for u, v in self.groups)
        self.row, self.col = row, col

    def partner(self, group, flip, cross=0):
        hi, lo = flip // 2, flip % 2
        core = 1 - self.core if cross else self.core
        groups = [list(g) for g in self.groups]
        if hi:
            groups[group][0] = 1 - groups[group][0]
        if lo:
            groups[group][1] = 1 - groups[group][1]
        (xa, ya), (yb, za), (zb, xb) = groups
        x, y, z = ((2 * b + (a + b) % 2) for a, b in ((xa, xb), (ya, yb), (za, zb)))
        return (y * 2 + x // 2, z * 4 + (x % 2) * 2 + core)

    def other_core(self):
        return (self.row, self.col + 1 - 2 * self.core)

    def flipped(self, group, flip):
        hi, lo = self.groups[group]
        if flip // 2:
            hi = 1 - hi
        if flip % 2:
            lo = 1 - lo
        return hi * 2 + lo


def at_groups(turn, first=None, second=None, third=None):
    found = [slice(None)] * 3
    for k, value in enumerate((first, second, third)):
        if value is not None:
            found[(turn + k) % 3] = value
    return tuple(found)


def gather_phases(place, out, pieces, sems, base, phases=(0, 1, 2), meanwhile=None):
    send, recv = sems
    mine = out.at[place.core]
    started = []

    def copy(block, number, device):
        made = pltpu.make_async_remote_copy(
            src_ref=block, dst_ref=block, send_sem=send.at[number], recv_sem=recv.at[number],
            device_id=device, device_id_type=MESH,
        )
        made.start()
        started.append(made)
        return made

    def spot(piece, *values):
        rows, cols, turn = piece
        return mine.at[(*at_groups(turn, *values), rows, cols)]

    waiting = [[] for _ in pieces]
    for phase in phases[:-1]:
        for n, piece in enumerate(pieces):
            turn = piece[2]
            q = [place.q[(turn + k) % 3] for k in range(3)]
            for made in waiting[n]:
                made.wait_recv()
            waiting[n] = []
            group = (turn + 2 - phase) % 3
            block = spot(piece, *(q, q[:2])[phase])
            for flip in (1, 2, 3):
                number = base + GATHERS * n + phase * 3 + flip - 1
                waiting[n].append(copy(block, number, place.partner(group, flip)))
        if phase == phases[0] and meanwhile is not None:
            meanwhile()
    halves = (pl.ds(0, 2), pl.ds(2, 2))
    across, landed = [], []
    for n, piece in enumerate(pieces):
        turn = piece[2]
        for made in waiting[n]:
            made.wait_recv()
        first = base + GATHERS * n + 6
        own = place.q[turn]
        now = {}
        for k in range(2):
            for flip, half in ((2, k), (1, 1 - k)):
                block = spot(piece, own, halves[half])
                now[flip, half] = copy(block, first + 2 * (flip - 1) + half,
                                       place.partner(turn, flip))
        across.append(copy(spot(piece, own), first + 6, place.other_core()))
        landed.append(now)
    for flip, half, step in ((2, 0, 0), (1, 1, 0), (2, 1, 1), (1, 0, 1)):
        for n, piece in enumerate(pieces):
            turn = piece[2]
            first = base + GATHERS * n + 6
            landed[n][flip, half].wait_recv()
            block = spot(piece, place.flipped(turn, flip), halves[half])
            if step == 0:
                landed[n][3, half] = copy(block, first + 4 + half, place.partner(turn, 3 - flip))
            across.append(
                copy(block, first + 7 + 2 * (flip - 1) + half, place.other_core())
            )
    for half in range(2):
        for n, piece in enumerate(pieces):
            turn = piece[2]
            first = base + GATHERS * n + 6
            landed[n][3, half].wait_recv()
            block = spot(piece, place.flipped(turn, 3), halves[half])
            across.append(copy(block, first + 11 + half, place.other_core()))
    for made in across:
        made.wait_recv()
    for made in started:
        made.wait_send()


def greet(place):
    barrier = pltpu.get_barrier_semaphore()
    known = [place.other_core()]
    for group, both in ((0, True), (1, False), (2, True)):
        for flip in (1, 2, 3):
            known.append(place.partner(group, flip))
            if both:
                known.append(place.partner(group, flip, 1))
    for device in known:
        pl.semaphore_signal(barrier, inc=1, device_id=device, device_id_type=MESH)
    return len(known)


def joined(pairs):
    peak = pairs[0][0]
    for other, _ in pairs[1:]:
        peak = jnp.maximum(peak, other)
    total = pairs[0][1] * jnp.exp(pairs[0][0] - peak)
    for other, amount in pairs[1:]:
        total = total + amount * jnp.exp(other - peak)
    return peak, total


def join_columns(place, pairs, held, slots, send, recv, base):
    core = place.core
    started = []

    def copy(src, dst, number, device):
        made = pltpu.make_async_remote_copy(
            src_ref=src, dst_ref=dst, send_sem=send.at[number], recv_sem=recv.at[number],
            device_id=device, device_id_type=MESH,
        )
        made.start()
        started.append(made)
        return made

    def device(group, flip, cross):
        return place.other_core() if flip == 0 else place.partner(group, flip, cross)

    ways = [(flip, cross) for flip in range(4) for cross in range(2) if flip or cross]
    now = []
    for flip, cross in ways:
        k = 2 * flip + cross
        half = 1 - core if cross else core
        now.append(copy(pairs.at[half], slots.at[0, k], base + k, device(0, flip, cross)))
    for made in now:
        made.wait_recv()
    found = [(pairs[core, 0], pairs[core, 1])]
    found += [(slots[0, 2 * f + c, 0], slots[0, 2 * f + c, 1]) for f, c in ways]
    held[0, 0], held[0, 1] = joined(found)
    now = []
    for flip in (1, 2, 3):
        number = base + 8 + flip
        now.append(copy(held.at[0], slots.at[1, flip], number, device(1, flip, 0)))
    for made in now:
        made.wait_recv()
    found = [(held[0, 0], held[0, 1])]
    found += [(slots[1, flip, 0], slots[1, flip, 1]) for flip in (1, 2, 3)]
    held[1, 0], held[1, 1] = joined(found)
    now = []
    for flip, cross in ways:
        k = 2 * flip + cross
        now.append(copy(held.at[1], slots.at[2, k], base + 16 + k, device(2, flip, cross)))
    for made in now:
        made.wait_recv()
    found = [(held[1, 0], held[1, 1])]
    found += [(slots[2, 2 * flip, 0], slots[2, 2 * flip, 1]) for flip in (1, 2, 3)]
    own = joined(found)
    other = joined([(slots[2, 2 * flip + 1, 0], slots[2, 2 * flip + 1, 1]) for flip in range(4)])
    return own, other, started


def find_target(
    place, pieces, total_noise, target_ref, data, data_hi, data_lo, anchor, anchor_hi, anchor_lo,
    score, running, pairs, held, slots, send_sem, recv_sem, meanwhile,
):
    f32, bf16 = jnp.float32, jnp.bfloat16
    width = anchor.shape[1]
    chunks, _, chunk = score.shape
    total_data = chunks * chunk
    gather_phases(place, data, pieces, (send_sem, recv_sem), 0, meanwhile=meanwhile)
    x = anchor[...]
    noise_sq = jnp.sum(x * x, axis=1, keepdims=True)

    across = (((1,), (1,)), ((), ()))
    lanes = 128
    tiles = chunk // lanes
    running[...] = jnp.full_like(running, -jnp.inf)

    @pl.loop(0, chunks)
    def _(i):
        points = data[i // 8, (i // 2) % 4, pl.ds((i % 2) * 2, 2)].reshape(chunk, width)
        high = points.astype(bf16)
        low = (points - high.astype(f32)).astype(bf16)
        data_hi[i] = high
        data_lo[i] = low
        square = points * points
        part = square[:, :lanes]
        for k in range(1, width // lanes):
            part = part + square[:, k * lanes : (k + 1) * lanes]
        data_sq = jnp.sum(part.T, axis=0, keepdims=True)
        inner = lax.dot_general(anchor_hi[...], high, across, preferred_element_type=f32)
        inner += lax.dot_general(anchor_hi[...], low, across, preferred_element_type=f32)
        inner += lax.dot_general(anchor_lo[...], high, across, preferred_element_type=f32)
        cost = (noise_sq + data_sq - 2.0 * inner) * (1.0 / width)
        found = cost * (-1.0 / ENTROPY)
        score[i] = found
        peak = running[...]
        for k in range(tiles):
            peak = jnp.maximum(peak, found[:, k * lanes : (k + 1) * lanes])
        running[...] = peak

    peak = jnp.max(running[...], axis=1, keepdims=True)
    running[...] = jnp.zeros_like(running)

    @pl.loop(0, chunks)
    def _(i):
        e = jnp.exp(score[i] - peak)
        total = running[...]
        for k in range(tiles):
            total = total + e[:, k * lanes : (k + 1) * lanes]
        running[...] = total

    total = jnp.sum(running[...], axis=1, keepdims=True)
    row_lse = peak + jnp.log(total) - math.log(float(total_data))

    @pl.loop(0, chunks)
    def _(i):
        s = score[i] - row_lse
        col_peak = jnp.max(s, axis=0, keepdims=True)
        col_total = jnp.sum(jnp.exp(s - col_peak), axis=0, keepdims=True)
        for k in range(tiles):
            at = i * tiles + k
            cols = slice(k * lanes, (k + 1) * lanes)
            pairs[at // 16, 0, pl.ds(at % 16, 1), :] = col_peak[:, cols]
            pairs[at // 16, 1, pl.ds(at % 16, 1), :] = col_total[:, cols]

    base = GATHERS * len(pieces)
    own, other, started = join_columns(place, pairs, held, slots, send_sem, recv_sem, base)
    for made in started:
        made.wait_send()
    log_noise = math.log(float(total_noise))
    pairs[place.core, 0] = own[0] + jnp.log(own[1]) - log_noise
    pairs[1 - place.core, 0] = other[0] + jnp.log(other[1]) - log_noise
    running[...] = jnp.full_like(running, -jnp.inf)

    @pl.loop(0, chunks)
    def _(i):
        peak = running[...]
        for k in range(tiles):
            at = i * tiles + k
            cols = slice(k * lanes, (k + 1) * lanes)
            s = score[i, :, cols] - pairs[at // 16, 0, pl.ds(at % 16, 1), :]
            score[i, :, cols] = s
            peak = jnp.maximum(peak, s)
        running[...] = peak

    peak = jnp.max(running[...], axis=1, keepdims=True)
    running[...] = jnp.zeros_like(running)
    target_ref[...] = jnp.zeros_like(target_ref)

    @pl.loop(0, chunks)
    def _(i):
        weights = jnp.exp(score[i] - peak).astype(bf16)
        total = running[...]
        for k in range(tiles):
            total = total + weights[:, k * lanes : (k + 1) * lanes].astype(f32)
        running[...] = total
        target_ref[...] += jnp.dot(
            weights, data_hi[i], preferred_element_type=f32
        ) + jnp.dot(weights, data_lo[i], preferred_element_type=f32)

    target_ref[...] = target_ref[...] / jnp.sum(running[...], axis=1, keepdims=True)


def sum_grads(
    place, pieces, in_ref, out_ref, acc, from_core, slot_0, slot_1, slot_2, send_sem, recv_sem
):
    core = place.core
    count = len(pieces)

    def copy(src, dst, number, device):
        made = pltpu.make_async_remote_copy(
            src_ref=src, dst_ref=dst, send_sem=send_sem.at[number], recv_sem=recv_sem.at[number],
            device_id=device, device_id_type=MESH,
        )
        made.start()
        started.append(made)
        return made

    every = slice(None)
    other = 1 - core
    started = []
    first = []
    for n, (_, cols, turn) in enumerate(pieces):
        first.append(copy(in_ref.at[other, :, :, :, :, cols], from_core.at[:, :, :, :, cols], n,
                          place.other_core()))
    base = count
    halves = (pl.ds(0, 2), pl.ds(2, 2))
    landed = []

    def part(turn, flip, half, cols):
        lead = at_groups(turn, place.flipped(turn, flip), halves[half])
        return (*lead, every, cols)

    for n, (_, cols, turn) in enumerate(pieces):
        first[n].wait_recv()
        wide = slice(0, cols.stop - cols.start)

        @pl.loop(0, 16)
        def _(i, cols=cols):
            a, b = i // 4, i % 4
            acc[a, b, :, :, cols] = in_ref[core, a, b, :, :, cols] + from_core[a, b, :, :, cols]

        now = {}
        for flip, half, kind in ((3, 0, 0), (3, 1, 0), (1, 0, 1), (2, 1, 1)):
            way = 1 + half if kind == 0 else flip
            number = base + n * 6 + 2 * kind + (way - 1)
            dst = slot_0.at[n, 2 * kind + way - 1]
            now[kind, way] = copy(
                acc.at[part(turn, flip, half, cols)],
                view(dst, turn, wide), number, place.partner(turn, way),
            )
        landed.append(now)
    for way, half in ((1, 0), (2, 1)):
        for n, (_, cols, turn) in enumerate(pieces):
            wide = slice(0, cols.stop - cols.start)
            landed[n][0, way].wait_recv()
            spot = part(turn, 3 - way, half, cols)
            acc[spot] = acc[spot] + view(slot_0.at[n, way - 1], turn, wide)[...]
            number = base + n * 6 + 4 + (2 - way)
            landed[n][2, 3 - way] = copy(
                acc.at[spot], view(slot_0.at[n, 4 + 2 - way], turn, wide), number,
                place.partner(turn, 3 - way),
            )
    base += 6 * count
    for n, (_, cols, turn) in enumerate(pieces):
        wide = slice(0, cols.stop - cols.start)
        for kind in (1, 2):
            for way in (1, 2):
                landed[n][kind, way].wait_recv()
        for half in (0, 1):
            spot = part(turn, 0, half, cols)
            one, two = (2, 5) if half == 0 else (3, 4)
            acc[spot] = acc[spot] + (
                view(slot_0.at[n, one], turn, wide)[...] + view(slot_0.at[n, two], turn, wide)[...]
            )
    waiting = [[] for _ in pieces]
    for n, (_, cols, turn) in enumerate(pieces):
        wide = slice(0, cols.stop - cols.start)
        group = (turn + 1) % 3
        for flip in (1, 2, 3):
            src = acc.at[(*at_groups(turn, place.q[turn], place.flipped(group, flip)), every, cols)]
            waiting[n].append(
                copy(src, slot_1.at[n, flip - 1, :, :, wide], base + n * 3 + flip - 1,
                     place.partner(group, flip))
            )
    base += 3 * count
    for n, (_, cols, turn) in enumerate(pieces):
        wide = slice(0, cols.stop - cols.start)
        for made in waiting[n]:
            made.wait_recv()
        waiting[n] = []
        group = (turn + 2) % 3
        spot = (*at_groups(turn, place.q[turn], place.q[(turn + 1) % 3]), every, cols)
        acc[spot] = (acc[spot] + slot_1[n, 0, :, :, wide]) + (
            slot_1[n, 1, :, :, wide] + slot_1[n, 2, :, :, wide]
        )
        for flip in (1, 2, 3):
            waiting[n].append(
                copy(acc.at[spot], slot_2.at[n, flip - 1, :, :, wide], base + n * 3 + flip - 1,
                     place.partner(group, flip))
            )
    base += 3 * count
    for n, (_, cols, turn) in enumerate(pieces):
        wide = slice(0, cols.stop - cols.start)
        for made in waiting[n]:
            made.wait_recv()
        spot = (*at_groups(turn, place.q[turn], place.q[(turn + 1) % 3]), every, cols)
        out_ref[(core, *spot)] = (acc[spot] + slot_2[n, 0, :, :, wide]) + (
            slot_2[n, 1, :, :, wide] + slot_2[n, 2, :, :, wide]
        )
    gather_phases(place, out_ref, pieces, (send_sem, recv_sem), base, (1, 2))
    for made in started:
        made.wait_send()


def view(ref, turn, wide):
    shape = [None, None]
    where = [(turn + 1) % 3, (turn + 2) % 3]
    shape = (2, 4) if where[0] < where[1] else (4, 2)
    return ref.reshape(*shape, *ref.shape[1:]).at[:, :, :, wide]


def spread(rows, steps_each):
    count, width = rows.shape
    wide = jnp.broadcast_to(rows[:, None, :], (count, steps_each, width))
    return wide.reshape(count * steps_each, width)


def train(
    scale, points, steps_each, anchor_ref, target_ref, tvals_ref, shift_ref, w_in_ref, w_out_ref,
    w_back_ref, predicted_ref, grads_ref, mixed_ref, hidden_ref, delta_ref, delta_pre_ref,
):
    block = points * steps_each
    width, hid_width = w_in_ref.shape
    blocks = anchor_ref.shape[0] // points
    f32, bf16 = jnp.float32, jnp.bfloat16
    contract = (((0,), (0,)), ((), ()))
    lanes = 128

    def forward(b, slot):
        here = pl.ds(pl.multiple_of(b * points, points), points)
        anchor, target = anchor_ref[here, :], target_ref[here, :]
        tvals = tvals_ref[pl.ds(pl.multiple_of(b * block, block), block), :]
        parts = []
        for k in range(width // lanes):
            cols = slice(k * lanes, (k + 1) * lanes)
            x, y = spread(anchor[:, cols], steps_each), spread(target[:, cols], steps_each)
            parts.append(((1.0 - tvals) * x + tvals * y).astype(bf16))
        mixed = jnp.concatenate(parts, axis=1)
        mixed_ref[slot] = mixed
        pre = jnp.dot(mixed, w_in_ref[...], preferred_element_type=f32)
        shift = jnp.concatenate(
            [tvals * shift_ref[:, k * lanes : (k + 1) * lanes] for k in range(hid_width // lanes)],
            axis=1,
        )
        pre = pre + shift
        sig = 0.5 * jnp.tanh(0.5 * pre) + 0.5
        hidden = (pre * sig).astype(bf16)
        slope = sig * (1.0 + pre * (1.0 - sig))
        hidden_ref[slot] = hidden
        output = jnp.dot(hidden, w_out_ref[...], preferred_element_type=f32)
        predicted_ref[pl.ds(pl.multiple_of(b * block, block), block), :] = output.astype(bf16)
        velocity = spread(target - anchor, steps_each)
        delta = ((output - velocity) * scale).astype(bf16)
        delta_ref[slot] = delta
        back = jnp.dot(delta, w_back_ref[...], preferred_element_type=f32)
        delta_pre_ref[slot] = (back * slope).astype(bf16)

    def add_grads(slot):
        grads_ref[0] += lax.dot_general(
            mixed_ref[slot], delta_pre_ref[slot], contract, preferred_element_type=f32
        )
        for k in range(hid_width // width):
            cols = slice(k * width, (k + 1) * width)
            grads_ref[1, :, cols] += lax.dot_general(
                hidden_ref[slot, :, cols], delta_ref[slot], contract, preferred_element_type=f32
            )

    forward(0, 0)

    @pl.loop(0, blocks // 2 - 1)
    def _(j):
        forward(2 * j + 1, 1)
        add_grads(0)
        forward(2 * j + 2, 0)
        add_grads(1)

    forward(blocks - 1, 1)
    add_grads(0)
    add_grads(1)


def step_kernel(
    data_pieces, grad_pieces, total_noise, points, data_ref, noise_ref, times_ref, shift_ref,
    w_in_ref, w_out_ref, predicted_ref, summed, data, data_hi, data_lo, anchor,
    anchor_hi, anchor_lo, score, running, pairs, held, slots, target, w_in, w_out, w_back, steps,
    tvals, mixed, hidden, delta, delta_pre, grads, acc, from_core, slot_0, slot_1,
    slot_2, local_sem, send_sem, recv_sem, grad_send_sem, grad_recv_sem,
):
    place = Place()
    f32, bf16 = jnp.float32, jnp.bfloat16
    rows = data.shape[4]
    share, width = anchor.shape
    hid_width = w_in.shape[1]
    steps_each = times_ref.shape[0]
    start = pl.multiple_of(place.row * rows, rows)
    first = pl.multiple_of(place.col * share, share)
    loads = [
        pltpu.make_async_copy(source, to, local_sem.at[k])
        for k, (source, to) in enumerate((
            (data_ref.at[pl.ds(start, rows)], data.at[(place.core, *place.q)]),
            (noise_ref.at[pl.ds(first, share)], anchor),
            (w_out_ref, w_out),
            (w_in_ref, w_in),
        ))
    ]
    for load in loads:
        load.start()
    count = greet(place)
    block = points * steps_each

    def prepare():
        grads[...] = jnp.zeros_like(grads)
        steps[...] = times_ref[...].T

        @pl.loop(0, share // points)
        def _(b):
            here = pl.ds(pl.multiple_of(b * points, points), points)
            wide = spread(steps[here, :], steps_each)
            row = lax.broadcasted_iota(jnp.int32, wide.shape, 0)
            lane = lax.broadcasted_iota(jnp.int32, wide.shape, 1)
            own = jnp.where(row % steps_each == lane, wide, 0.0)
            value = jnp.sum(own, axis=1, keepdims=True)
            to = pl.ds(pl.multiple_of(b * block, block), block)
            tvals[to, :] = jnp.broadcast_to(value, (block, 128))

        for load in loads[1:]:
            load.wait()
        x = anchor[...]
        high = x.astype(bf16)
        anchor_hi[...] = high
        anchor_lo[...] = (x - high.astype(f32)).astype(bf16)
        for k in range(hid_width // 256):
            part = slice(k * 256, (k + 1) * 256)
            w_back[:, part] = w_out[part, :].T

    loads[0].wait()
    pl.semaphore_wait(pltpu.get_barrier_semaphore(), count)
    find_target(
        place, data_pieces, total_noise, target, data, data_hi, data_lo, anchor, anchor_hi,
        anchor_lo, score, running, pairs, held, slots, send_sem, recv_sem, prepare,
    )
    scale = 1.0 / math.sqrt(float(total_noise * steps_each))
    train(
        scale, points, steps_each, anchor, target, tvals, shift_ref, w_in, w_out, w_back,
        predicted_ref, grads, mixed, hidden, delta, delta_pre,
    )
    sum_grads(
        place, grad_pieces, grads.reshape(summed.shape), summed, acc, from_core, slot_0, slot_1,
        slot_2, grad_send_sem, grad_recv_sem,
    )


def store_kernel(predicted, summed, predicted_ref, grad_in_ref, grad_out_ref, sem):
    width, hid_width = grad_in_ref.shape
    result = summed.reshape(2, width, hid_width)
    moves = [(predicted, predicted_ref), (result.at[0], grad_in_ref)]
    for k in range(hid_width // width):
        part = slice(k * width, (k + 1) * width)
        moves.append((result.at[1, :, part], grad_out_ref.at[part]))
    made = [pltpu.make_async_copy(a, b, sem.at[k]) for k, (a, b) in enumerate(moves)]
    for copy in made:
        copy.start()
    for copy in made:
        copy.wait()


def on_device(noise_points, data_points, times, time_shift, weight_in, weight_out):
    count_row = lax.axis_size("row")
    count_col = lax.axis_size("col")
    total_noise = noise_points.shape[0] * count_row
    total_data = data_points.shape[0] * count_col
    width, hid_width = weight_in.shape
    share, steps_each = times.shape
    rows = data_points.shape[0] // count_row
    chunk = 8 * rows
    chunks = total_data // chunk
    points = 32
    block = points * steps_each
    quarter, tile = rows // 4, width // 4
    every = slice(None)
    last = slice(3 * quarter, rows)
    data_pieces = (
        (slice(0, quarter), every, 0),
        (slice(quarter, 2 * quarter), every, 1),
        (slice(2 * quarter, 3 * quarter), every, 2),
        (last, slice(0, tile), 0),
        (last, slice(tile, 2 * tile), 1),
        (last, slice(2 * tile, width), 2),
    )
    third = 128 * -(-hid_width // 384)
    grad_pieces = (
        (every, slice(0, third), 0),
        (every, slice(third, 2 * third), 1),
        (every, slice(2 * third, hid_width), 2),
    )
    parts = len(grad_pieces)
    copies = GATHERS * len(data_pieces) + 24
    grad_copies = (1 + 6 + 6 + GATHERS) * len(grad_pieces)
    f32, bf16 = jnp.float32, jnp.bfloat16
    pair = (2, total_data // 256, 128)
    units = (4, 4, 4, width // 64, hid_width)
    far = pl.BlockSpec(memory_space=pl.ANY)
    near = pl.BlockSpec(memory_space=pltpu.VMEM)
    predicted, summed = pl.pallas_call(
        functools.partial(step_kernel, data_pieces, grad_pieces, total_noise, points),
        out_shape=(
            pltpu.VMEM((share * steps_each, width), bf16),
            pltpu.VMEM((2, *units), f32),
        ),
        in_specs=[far, far, near, near, far, far],
        out_specs=(near, near),
        scratch_shapes=[
            pltpu.VMEM((2, 4, 4, 4, rows, width), f32),
            pltpu.VMEM((chunks, chunk, width), bf16),
            pltpu.VMEM((chunks, chunk, width), bf16),
            pltpu.VMEM((share, width), f32),
            pltpu.VMEM((share, width), bf16),
            pltpu.VMEM((share, width), bf16),
            pltpu.VMEM((chunks, share, chunk), f32),
            pltpu.VMEM((share, 128), f32),
            pltpu.VMEM((2, *pair), f32),
            pltpu.VMEM((2, *pair), f32),
            pltpu.VMEM((3, 8, *pair), f32),
            pltpu.VMEM((share, width), f32),
            pltpu.VMEM((width, hid_width), bf16),
            pltpu.VMEM((hid_width, width), bf16),
            pltpu.VMEM((width, hid_width), bf16),
            pltpu.VMEM((share, steps_each), f32),
            pltpu.VMEM((share * steps_each, 128), f32),
            pltpu.VMEM((2, block, width), bf16),
            pltpu.VMEM((2, block, hid_width), bf16),
            pltpu.VMEM((2, block, width), bf16),
            pltpu.VMEM((2, block, hid_width), bf16),
            pltpu.VMEM((2, width, hid_width), f32),
            pltpu.VMEM(units, f32),
            pltpu.VMEM(units, f32),
            pltpu.VMEM((parts, 6, 8, width // 64, third), f32),
            pltpu.VMEM((parts, 3, 4, width // 64, third), f32),
            pltpu.VMEM((parts, 3, 4, width // 64, third), f32),
            pltpu.SemaphoreType.DMA((4,)),
            pltpu.SemaphoreType.DMA((copies,)),
            pltpu.SemaphoreType.DMA((copies,)),
            pltpu.SemaphoreType.DMA((grad_copies,)),
            pltpu.SemaphoreType.DMA((grad_copies,)),
        ],
        compiler_params=pltpu.CompilerParams(
            collective_id=1, has_side_effects=True, vmem_limit_bytes=VMEM_CAP
        ),
        name="step",
    )(data_points, noise_points, times.T, time_shift.reshape(1, hid_width), weight_in, weight_out)
    return pl.pallas_call(
        store_kernel,
        out_shape=(
            jax.ShapeDtypeStruct((share * steps_each, width), bf16),
            jax.ShapeDtypeStruct((width, hid_width), f32),
            jax.ShapeDtypeStruct((hid_width, width), f32),
        ),
        in_specs=[near, near],
        out_specs=(far, far, far),
        scratch_shapes=[pltpu.SemaphoreType.DMA((2 + hid_width // width,))],
        compiler_params=pltpu.CompilerParams(vmem_limit_bytes=1024 * 1024),
        name="store",
    )(*(pltpu.with_memory_space_constraint(a, pltpu.VMEM) for a in (predicted, summed)))


def solution(mesh):
    in_specs = (P("row", None), P("col", None), P(("row", "col"), None), P(), P(), P())
    out_specs = (P(("row", "col"), None), P(), P())
    return jax.shard_map(
        on_device, mesh=mesh, in_specs=in_specs, out_specs=out_specs, check_vma=False
    )
```

```python
import functools
import math

import jax
import jax.numpy as jnp
from jax import lax
from jax.experimental import pallas as pl
from jax.experimental.pallas import tpu as pltpu
from jax.sharding import PartitionSpec as P

ENTROPY = 0.05
MESH = pl.DeviceIdType.MESH
VMEM_CAP = 54 * 1024 * 1024
GATHERS = 19


class Place:
    def __init__(self):
        row, col = lax.axis_index("row"), lax.axis_index("col")
        self.core = col % 2
        x = (row % 2) * 2 + (col // 2) % 2
        y = row // 2
        z = col // 4
        self.bits = []
        for pos in (x, y, z):
            self.bits.append(((pos + pos // 2) % 2, pos // 2))
        (xa, xb), (ya, yb), (za, zb) = self.bits
        self.groups = ((xa, ya), (yb, za), (zb, xb))
        self.q = tuple(u * 2 + v for u, v in self.groups)
        self.row, self.col = row, col

    def partner(self, group, flip, cross=0):
        hi, lo = flip // 2, flip % 2
        core = 1 - self.core if cross else self.core
        groups = [list(g) for g in self.groups]
        if hi:
            groups[group][0] = 1 - groups[group][0]
        if lo:
            groups[group][1] = 1 - groups[group][1]
        (xa, ya), (yb, za), (zb, xb) = groups
        x, y, z = ((2 * b + (a + b) % 2) for a, b in ((xa, xb), (ya, yb), (za, zb)))
        return (y * 2 + x // 2, z * 4 + (x % 2) * 2 + core)

    def other_core(self):
        return (self.row, self.col + 1 - 2 * self.core)

    def flipped(self, group, flip):
        hi, lo = self.groups[group]
        if flip // 2:
            hi = 1 - hi
        if flip % 2:
            lo = 1 - lo
        return hi * 2 + lo


def at_groups(turn, first=None, second=None, third=None):
    found = [slice(None)] * 3
    for k, value in enumerate((first, second, third)):
        if value is not None:
            found[(turn + k) % 3] = value
    return tuple(found)


def gather_phases(place, out, pieces, sems, base, phases=(0, 1, 2), meanwhile=None):
    send, recv = sems
    mine = out.at[place.core]
    started = []

    def copy(block, number, device):
        made = pltpu.make_async_remote_copy(
            src_ref=block, dst_ref=block, send_sem=send.at[number], recv_sem=recv.at[number],
            device_id=device, device_id_type=MESH,
        )
        made.start()
        started.append(made)
        return made

    def spot(piece, *values):
        rows, cols, turn = piece
        return mine.at[(*at_groups(turn, *values), rows, cols)]

    waiting = [[] for _ in pieces]
    for phase in phases[:-1]:
        for n, piece in enumerate(pieces):
            turn = piece[2]
            q = [place.q[(turn + k) % 3] for k in range(3)]
            for made in waiting[n]:
                made.wait_recv()
            waiting[n] = []
            group = (turn + 2 - phase) % 3
            block = spot(piece, *(q, q[:2])[phase])
            for flip in (1, 2, 3):
                number = base + GATHERS * n + phase * 3 + flip - 1
                waiting[n].append(copy(block, number, place.partner(group, flip)))
        if phase == phases[0] and meanwhile is not None:
            meanwhile()
    halves = (pl.ds(0, 2), pl.ds(2, 2))
    across, landed = [], []
    for n, piece in enumerate(pieces):
        turn = piece[2]
        for made in waiting[n]:
            made.wait_recv()
        first = base + GATHERS * n + 6
        own = place.q[turn]
        now = {}
        for k in range(2):
            for flip, half in ((2, k), (1, 1 - k)):
                block = spot(piece, own, halves[half])
                now[flip, half] = copy(block, first + 2 * (flip - 1) + half,
                                       place.partner(turn, flip))
        across.append(copy(spot(piece, own), first + 6, place.other_core()))
        landed.append(now)
    for flip, half, step in ((2, 0, 0), (1, 1, 0), (2, 1, 1), (1, 0, 1)):
        for n, piece in enumerate(pieces):
            turn = piece[2]
            first = base + GATHERS * n + 6
            landed[n][flip, half].wait_recv()
            block = spot(piece, place.flipped(turn, flip), halves[half])
            if step == 0:
                landed[n][3, half] = copy(block, first + 4 + half, place.partner(turn, 3 - flip))
            across.append(
                copy(block, first + 7 + 2 * (flip - 1) + half, place.other_core())
            )
    for half in range(2):
        for n, piece in enumerate(pieces):
            turn = piece[2]
            first = base + GATHERS * n + 6
            landed[n][3, half].wait_recv()
            block = spot(piece, place.flipped(turn, 3), halves[half])
            across.append(copy(block, first + 11 + half, place.other_core()))
    for made in across:
        made.wait_recv()
    for made in started:
        made.wait_send()


def greet(place):
    barrier = pltpu.get_barrier_semaphore()
    known = [place.other_core()]
    for group, both in ((0, True), (1, False), (2, True)):
        for flip in (1, 2, 3):
            known.append(place.partner(group, flip))
            if both:
                known.append(place.partner(group, flip, 1))
    for device in known:
        pl.semaphore_signal(barrier, inc=1, device_id=device, device_id_type=MESH)
    return len(known)


def joined(pairs):
    peak = pairs[0][0]
    for other, _ in pairs[1:]:
        peak = jnp.maximum(peak, other)
    total = pairs[0][1] * jnp.exp(pairs[0][0] - peak)
    for other, amount in pairs[1:]:
        total = total + amount * jnp.exp(other - peak)
    return peak, total


def join_columns(place, pairs, held, slots, send, recv, base):
    core = place.core
    started = []

    def copy(src, dst, number, device):
        made = pltpu.make_async_remote_copy(
            src_ref=src, dst_ref=dst, send_sem=send.at[number], recv_sem=recv.at[number],
            device_id=device, device_id_type=MESH,
        )
        made.start()
        started.append(made)
        return made

    def device(group, flip, cross):
        return place.other_core() if flip == 0 else place.partner(group, flip, cross)

    ways = [(flip, cross) for flip in range(4) for cross in range(2) if flip or cross]
    now = []
    for flip, cross in ways:
        k = 2 * flip + cross
        half = 1 - core if cross else core
        now.append(copy(pairs.at[half], slots.at[0, k], base + k, device(0, flip, cross)))
    for made in now:
        made.wait_recv()
    found = [(pairs[core, 0], pairs[core, 1])]
    found += [(slots[0, 2 * f + c, 0], slots[0, 2 * f + c, 1]) for f, c in ways]
    held[0, 0], held[0, 1] = joined(found)
    now = []
    for flip in (1, 2, 3):
        number = base + 8 + flip
        now.append(copy(held.at[0], slots.at[1, flip], number, device(1, flip, 0)))
    for made in now:
        made.wait_recv()
    found = [(held[0, 0], held[0, 1])]
    found += [(slots[1, flip, 0], slots[1, flip, 1]) for flip in (1, 2, 3)]
    held[1, 0], held[1, 1] = joined(found)
    now = []
    for flip, cross in ways:
        k = 2 * flip + cross
        now.append(copy(held.at[1], slots.at[2, k], base + 16 + k, device(2, flip, cross)))
    for made in now:
        made.wait_recv()
    found = [(held[1, 0], held[1, 1])]
    found += [(slots[2, 2 * flip, 0], slots[2, 2 * flip, 1]) for flip in (1, 2, 3)]
    own = joined(found)
    other = joined([(slots[2, 2 * flip + 1, 0], slots[2, 2 * flip + 1, 1]) for flip in range(4)])
    return own, other, started


def find_target(
    place, pieces, total_noise, target_ref, data, data_hi, data_lo, anchor, anchor_hi, anchor_lo,
    score, running, pairs, held, slots, send_sem, recv_sem, meanwhile,
):
    f32, bf16 = jnp.float32, jnp.bfloat16
    width = anchor.shape[1]
    chunks, _, chunk = score.shape
    total_data = chunks * chunk
    gather_phases(place, data, pieces, (send_sem, recv_sem), 0, meanwhile=meanwhile)
    x = anchor[...]
    noise_sq = jnp.sum(x * x, axis=1, keepdims=True)

    across = (((1,), (1,)), ((), ()))
    lanes = 128
    tiles = chunk // lanes
    running[...] = jnp.full_like(running, -jnp.inf)

    @pl.loop(0, chunks, unroll=2)
    def _(i):
        points = data[i // 8, (i // 2) % 4, pl.ds((i % 2) * 2, 2)].reshape(chunk, width)
        high = points.astype(bf16)
        low = (points - high.astype(f32)).astype(bf16)
        data_hi[i] = high
        data_lo[i] = low
        square = points * points
        part = square[:, :lanes]
        for k in range(1, width // lanes):
            part = part + square[:, k * lanes : (k + 1) * lanes]
        data_sq = jnp.sum(part.T, axis=0, keepdims=True)
        inner = lax.dot_general(anchor_hi[...], high, across, preferred_element_type=f32)
        inner += lax.dot_general(anchor_hi[...], low, across, preferred_element_type=f32)
        inner += lax.dot_general(anchor_lo[...], high, across, preferred_element_type=f32)
        cost = (noise_sq + data_sq - 2.0 * inner) * (1.0 / width)
        found = cost * (-1.0 / ENTROPY)
        score[i] = found
        peak = running[...]
        for k in range(tiles):
            peak = jnp.maximum(peak, found[:, k * lanes : (k + 1) * lanes])
        running[...] = peak

    peak = jnp.max(running[...], axis=1, keepdims=True)
    running[...] = jnp.zeros_like(running)

    @pl.loop(0, chunks, unroll=2)
    def _(i):
        e = jnp.exp(score[i] - peak)
        total = running[...]
        for k in range(tiles):
            total = total + e[:, k * lanes : (k + 1) * lanes]
        running[...] = total

    total = jnp.sum(running[...], axis=1, keepdims=True)
    row_lse = peak + jnp.log(total) - math.log(float(total_data))

    @pl.loop(0, chunks, unroll=2)
    def _(i):
        s = score[i] - row_lse
        col_peak = jnp.max(s, axis=0, keepdims=True)
        col_total = jnp.sum(jnp.exp(s - col_peak), axis=0, keepdims=True)
        for k in range(tiles):
            at = i * tiles + k
            cols = slice(k * lanes, (k + 1) * lanes)
            pairs[at // 16, 0, pl.ds(at % 16, 1), :] = col_peak[:, cols]
            pairs[at // 16, 1, pl.ds(at % 16, 1), :] = col_total[:, cols]

    base = GATHERS * len(pieces)
    own, other, started = join_columns(place, pairs, held, slots, send_sem, recv_sem, base)
    for made in started:
        made.wait_send()
    log_noise = math.log(float(total_noise))
    pairs[place.core, 0] = own[0] + jnp.log(own[1]) - log_noise
    pairs[1 - place.core, 0] = other[0] + jnp.log(other[1]) - log_noise
    running[...] = jnp.full_like(running, -jnp.inf)

    @pl.loop(0, chunks, unroll=2)
    def _(i):
        peak = running[...]
        for k in range(tiles):
            at = i * tiles + k
            cols = slice(k * lanes, (k + 1) * lanes)
            s = score[i, :, cols] - pairs[at // 16, 0, pl.ds(at % 16, 1), :]
            score[i, :, cols] = s
            peak = jnp.maximum(peak, s)
        running[...] = peak

    peak = jnp.max(running[...], axis=1, keepdims=True)
    running[...] = jnp.zeros_like(running)
    target_ref[...] = jnp.zeros_like(target_ref)

    @pl.loop(0, chunks, unroll=2)
    def _(i):
        weights = jnp.exp(score[i] - peak).astype(bf16)
        total = running[...]
        for k in range(tiles):
            total = total + weights[:, k * lanes : (k + 1) * lanes].astype(f32)
        running[...] = total
        target_ref[...] += jnp.dot(
            weights, data_hi[i], preferred_element_type=f32
        ) + jnp.dot(weights, data_lo[i], preferred_element_type=f32)

    target_ref[...] = target_ref[...] / jnp.sum(running[...], axis=1, keepdims=True)


def sum_grads(
    place, pieces, in_ref, out_ref, acc, from_core, slot_0, slot_1, slot_2, send_sem, recv_sem
):
    core = place.core
    count = len(pieces)

    def copy(src, dst, number, device):
        made = pltpu.make_async_remote_copy(
            src_ref=src, dst_ref=dst, send_sem=send_sem.at[number], recv_sem=recv_sem.at[number],
            device_id=device, device_id_type=MESH,
        )
        made.start()
        started.append(made)
        return made

    every = slice(None)
    other = 1 - core
    started = []
    first = []
    for n, (_, cols, turn) in enumerate(pieces):
        first.append(copy(in_ref.at[other, :, :, :, :, cols], from_core.at[:, :, :, :, cols], n,
                          place.other_core()))
    base = count
    halves = (pl.ds(0, 2), pl.ds(2, 2))
    landed = []

    def part(turn, flip, half, cols):
        lead = at_groups(turn, place.flipped(turn, flip), halves[half])
        return (*lead, every, cols)

    for n, (_, cols, turn) in enumerate(pieces):
        first[n].wait_recv()
        wide = slice(0, cols.stop - cols.start)

        @pl.loop(0, 16)
        def _(i, cols=cols):
            a, b = i // 4, i % 4
            acc[a, b, :, :, cols] = in_ref[core, a, b, :, :, cols] + from_core[a, b, :, :, cols]

        now = {}
        for flip, half, kind in ((3, 0, 0), (3, 1, 0), (1, 0, 1), (2, 1, 1)):
            way = 1 + half if kind == 0 else flip
            number = base + n * 6 + 2 * kind + (way - 1)
            dst = slot_0.at[n, 2 * kind + way - 1]
            now[kind, way] = copy(
                acc.at[part(turn, flip, half, cols)],
                view(dst, turn, wide), number, place.partner(turn, way),
            )
        landed.append(now)
    for way, half in ((1, 0), (2, 1)):
        for n, (_, cols, turn) in enumerate(pieces):
            wide = slice(0, cols.stop - cols.start)
            landed[n][0, way].wait_recv()
            spot = part(turn, 3 - way, half, cols)
            acc[spot] = acc[spot] + view(slot_0.at[n, way - 1], turn, wide)[...]
            number = base + n * 6 + 4 + (2 - way)
            landed[n][2, 3 - way] = copy(
                acc.at[spot], view(slot_0.at[n, 4 + 2 - way], turn, wide), number,
                place.partner(turn, 3 - way),
            )
    base += 6 * count
    for n, (_, cols, turn) in enumerate(pieces):
        wide = slice(0, cols.stop - cols.start)
        for kind in (1, 2):
            for way in (1, 2):
                landed[n][kind, way].wait_recv()
        for half in (0, 1):
            spot = part(turn, 0, half, cols)
            one, two = (2, 5) if half == 0 else (3, 4)
            acc[spot] = acc[spot] + (
                view(slot_0.at[n, one], turn, wide)[...] + view(slot_0.at[n, two], turn, wide)[...]
            )
    waiting = [[] for _ in pieces]
    for n, (_, cols, turn) in enumerate(pieces):
        wide = slice(0, cols.stop - cols.start)
        group = (turn + 1) % 3
        for flip in (1, 2, 3):
            src = acc.at[(*at_groups(turn, place.q[turn], place.flipped(group, flip)), every, cols)]
            waiting[n].append(
                copy(src, slot_1.at[n, flip - 1, :, :, wide], base + n * 3 + flip - 1,
                     place.partner(group, flip))
            )
    base += 3 * count
    for n, (_, cols, turn) in enumerate(pieces):
        wide = slice(0, cols.stop - cols.start)
        for made in waiting[n]:
            made.wait_recv()
        waiting[n] = []
        group = (turn + 2) % 3
        spot = (*at_groups(turn, place.q[turn], place.q[(turn + 1) % 3]), every, cols)
        acc[spot] = (acc[spot] + slot_1[n, 0, :, :, wide]) + (
            slot_1[n, 1, :, :, wide] + slot_1[n, 2, :, :, wide]
        )
        for flip in (1, 2, 3):
            waiting[n].append(
                copy(acc.at[spot], slot_2.at[n, flip - 1, :, :, wide], base + n * 3 + flip - 1,
                     place.partner(group, flip))
            )
    base += 3 * count
    for n, (_, cols, turn) in enumerate(pieces):
        wide = slice(0, cols.stop - cols.start)
        for made in waiting[n]:
            made.wait_recv()
        spot = (*at_groups(turn, place.q[turn], place.q[(turn + 1) % 3]), every, cols)
        out_ref[(core, *spot)] = (acc[spot] + slot_2[n, 0, :, :, wide]) + (
            slot_2[n, 1, :, :, wide] + slot_2[n, 2, :, :, wide]
        )
    gather_phases(place, out_ref, pieces, (send_sem, recv_sem), base, (1, 2))
    for made in started:
        made.wait_send()


def view(ref, turn, wide):
    shape = [None, None]
    where = [(turn + 1) % 3, (turn + 2) % 3]
    shape = (2, 4) if where[0] < where[1] else (4, 2)
    return ref.reshape(*shape, *ref.shape[1:]).at[:, :, :, wide]


def spread(rows, steps_each):
    count, width = rows.shape
    wide = jnp.broadcast_to(rows[:, None, :], (count, steps_each, width))
    return wide.reshape(count * steps_each, width)


def train(
    scale, points, steps_each, anchor_ref, target_ref, tvals_ref, shift_ref, w_in_ref, w_out_ref,
    w_back_ref, predicted_ref, grads_ref, mixed_ref, hidden_ref, delta_ref, delta_pre_ref,
):
    block = points * steps_each
    width, hid_width = w_in_ref.shape
    blocks = anchor_ref.shape[0] // points
    f32, bf16 = jnp.float32, jnp.bfloat16
    contract = (((0,), (0,)), ((), ()))
    lanes = 128

    def forward(b, slot):
        here = pl.ds(pl.multiple_of(b * points, points), points)
        anchor, target = anchor_ref[here, :], target_ref[here, :]
        tvals = tvals_ref[pl.ds(pl.multiple_of(b * block, block), block), :]
        parts = []
        for k in range(width // lanes):
            cols = slice(k * lanes, (k + 1) * lanes)
            x, y = spread(anchor[:, cols], steps_each), spread(target[:, cols], steps_each)
            parts.append(((1.0 - tvals) * x + tvals * y).astype(bf16))
        mixed = jnp.concatenate(parts, axis=1)
        mixed_ref[slot] = mixed
        pre = jnp.dot(mixed, w_in_ref[...], preferred_element_type=f32)
        shift = jnp.concatenate(
            [tvals * shift_ref[:, k * lanes : (k + 1) * lanes] for k in range(hid_width // lanes)],
            axis=1,
        )
        pre = pre + shift
        sig = 0.5 * jnp.tanh(0.5 * pre) + 0.5
        hidden = (pre * sig).astype(bf16)
        slope = sig * (1.0 + pre * (1.0 - sig))
        hidden_ref[slot] = hidden
        output = jnp.dot(hidden, w_out_ref[...], preferred_element_type=f32)
        predicted_ref[pl.ds(pl.multiple_of(b * block, block), block), :] = output.astype(bf16)
        velocity = spread(target - anchor, steps_each)
        delta = ((output - velocity) * scale).astype(bf16)
        delta_ref[slot] = delta
        back = jnp.dot(delta, w_back_ref[...], preferred_element_type=f32)
        delta_pre_ref[slot] = (back * slope).astype(bf16)

    def add_grads(slot):
        grads_ref[0] += lax.dot_general(
            mixed_ref[slot], delta_pre_ref[slot], contract, preferred_element_type=f32
        )
        for k in range(hid_width // width):
            cols = slice(k * width, (k + 1) * width)
            grads_ref[1, :, cols] += lax.dot_general(
                hidden_ref[slot, :, cols], delta_ref[slot], contract, preferred_element_type=f32
            )

    forward(0, 0)

    @pl.loop(0, blocks // 2 - 1)
    def _(j):
        forward(2 * j + 1, 1)
        add_grads(0)
        forward(2 * j + 2, 0)
        add_grads(1)

    forward(blocks - 1, 1)
    add_grads(0)
    add_grads(1)


def step_kernel(
    data_pieces, grad_pieces, total_noise, points, data_ref, noise_ref, times_ref, shift_ref,
    w_in_ref, w_out_ref, predicted_ref, summed, data, data_hi, data_lo, anchor,
    anchor_hi, anchor_lo, score, running, pairs, held, slots, target, w_in, w_out, w_back, steps,
    tvals, mixed, hidden, delta, delta_pre, grads, acc, from_core, slot_0, slot_1,
    slot_2, local_sem, send_sem, recv_sem, grad_send_sem, grad_recv_sem,
):
    place = Place()
    f32, bf16 = jnp.float32, jnp.bfloat16
    rows = data.shape[4]
    share, width = anchor.shape
    hid_width = w_in.shape[1]
    steps_each = times_ref.shape[0]
    start = pl.multiple_of(place.row * rows, rows)
    first = pl.multiple_of(place.col * share, share)
    loads = [
        pltpu.make_async_copy(source, to, local_sem.at[k])
        for k, (source, to) in enumerate((
            (data_ref.at[pl.ds(start, rows)], data.at[(place.core, *place.q)]),
            (noise_ref.at[pl.ds(first, share)], anchor),
            (w_out_ref, w_out),
            (w_in_ref, w_in),
        ))
    ]
    for load in loads:
        load.start()
    count = greet(place)
    block = points * steps_each

    def prepare():
        grads[...] = jnp.zeros_like(grads)
        steps[...] = times_ref[...].T

        @pl.loop(0, share // points)
        def _(b):
            here = pl.ds(pl.multiple_of(b * points, points), points)
            wide = spread(steps[here, :], steps_each)
            row = lax.broadcasted_iota(jnp.int32, wide.shape, 0)
            lane = lax.broadcasted_iota(jnp.int32, wide.shape, 1)
            own = jnp.where(row % steps_each == lane, wide, 0.0)
            value = jnp.sum(own, axis=1, keepdims=True)
            to = pl.ds(pl.multiple_of(b * block, block), block)
            tvals[to, :] = jnp.broadcast_to(value, (block, 128))

        for load in loads[1:]:
            load.wait()
        x = anchor[...]
        high = x.astype(bf16)
        anchor_hi[...] = high
        anchor_lo[...] = (x - high.astype(f32)).astype(bf16)
        for k in range(hid_width // 256):
            part = slice(k * 256, (k + 1) * 256)
            w_back[:, part] = w_out[part, :].T

    loads[0].wait()
    pl.semaphore_wait(pltpu.get_barrier_semaphore(), count)
    find_target(
        place, data_pieces, total_noise, target, data, data_hi, data_lo, anchor, anchor_hi,
        anchor_lo, score, running, pairs, held, slots, send_sem, recv_sem, prepare,
    )
    scale = 1.0 / math.sqrt(float(total_noise * steps_each))
    train(
        scale, points, steps_each, anchor, target, tvals, shift_ref, w_in, w_out, w_back,
        predicted_ref, grads, mixed, hidden, delta, delta_pre,
    )
    sum_grads(
        place, grad_pieces, grads.reshape(summed.shape), summed, acc, from_core, slot_0, slot_1,
        slot_2, grad_send_sem, grad_recv_sem,
    )


def store_kernel(predicted, summed, predicted_ref, grad_in_ref, grad_out_ref, sem):
    width, hid_width = grad_in_ref.shape
    result = summed.reshape(2, width, hid_width)
    moves = [(predicted, predicted_ref), (result.at[0], grad_in_ref)]
    for k in range(hid_width // width):
        part = slice(k * width, (k + 1) * width)
        moves.append((result.at[1, :, part], grad_out_ref.at[part]))
    made = [pltpu.make_async_copy(a, b, sem.at[k]) for k, (a, b) in enumerate(moves)]
    for copy in made:
        copy.start()
    for copy in made:
        copy.wait()


def on_device(noise_points, data_points, times, time_shift, weight_in, weight_out):
    count_row = lax.axis_size("row")
    count_col = lax.axis_size("col")
    total_noise = noise_points.shape[0] * count_row
    total_data = data_points.shape[0] * count_col
    width, hid_width = weight_in.shape
    share, steps_each = times.shape
    rows = data_points.shape[0] // count_row
    chunk = 8 * rows
    chunks = total_data // chunk
    points = 32
    block = points * steps_each
    quarter, tile = rows // 4, width // 4
    every = slice(None)
    last = slice(3 * quarter, rows)
    data_pieces = (
        (slice(0, quarter), every, 0),
        (slice(quarter, 2 * quarter), every, 1),
        (slice(2 * quarter, 3 * quarter), every, 2),
        (last, slice(0, tile), 0),
        (last, slice(tile, 2 * tile), 1),
        (last, slice(2 * tile, width), 2),
    )
    third = 128 * -(-hid_width // 384)
    grad_pieces = (
        (every, slice(0, third), 0),
        (every, slice(third, 2 * third), 1),
        (every, slice(2 * third, hid_width), 2),
    )
    parts = len(grad_pieces)
    copies = GATHERS * len(data_pieces) + 24
    grad_copies = (1 + 6 + 6 + GATHERS) * len(grad_pieces)
    f32, bf16 = jnp.float32, jnp.bfloat16
    pair = (2, total_data // 256, 128)
    units = (4, 4, 4, width // 64, hid_width)
    far = pl.BlockSpec(memory_space=pl.ANY)
    near = pl.BlockSpec(memory_space=pltpu.VMEM)
    predicted, summed = pl.pallas_call(
        functools.partial(step_kernel, data_pieces, grad_pieces, total_noise, points),
        out_shape=(
            pltpu.VMEM((share * steps_each, width), bf16),
            pltpu.VMEM((2, *units), f32),
        ),
        in_specs=[far, far, near, near, far, far],
        out_specs=(near, near),
        scratch_shapes=[
            pltpu.VMEM((2, 4, 4, 4, rows, width), f32),
            pltpu.VMEM((chunks, chunk, width), bf16),
            pltpu.VMEM((chunks, chunk, width), bf16),
            pltpu.VMEM((share, width), f32),
            pltpu.VMEM((share, width), bf16),
            pltpu.VMEM((share, width), bf16),
            pltpu.VMEM((chunks, share, chunk), f32),
            pltpu.VMEM((share, 128), f32),
            pltpu.VMEM((2, *pair), f32),
            pltpu.VMEM((2, *pair), f32),
            pltpu.VMEM((3, 8, *pair), f32),
            pltpu.VMEM((share, width), f32),
            pltpu.VMEM((width, hid_width), bf16),
            pltpu.VMEM((hid_width, width), bf16),
            pltpu.VMEM((width, hid_width), bf16),
            pltpu.VMEM((share, steps_each), f32),
            pltpu.VMEM((share * steps_each, 128), f32),
            pltpu.VMEM((2, block, width), bf16),
            pltpu.VMEM((2, block, hid_width), bf16),
            pltpu.VMEM((2, block, width), bf16),
            pltpu.VMEM((2, block, hid_width), bf16),
            pltpu.VMEM((2, width, hid_width), f32),
            pltpu.VMEM(units, f32),
            pltpu.VMEM(units, f32),
            pltpu.VMEM((parts, 6, 8, width // 64, third), f32),
            pltpu.VMEM((parts, 3, 4, width // 64, third), f32),
            pltpu.VMEM((parts, 3, 4, width // 64, third), f32),
            pltpu.SemaphoreType.DMA((4,)),
            pltpu.SemaphoreType.DMA((copies,)),
            pltpu.SemaphoreType.DMA((copies,)),
            pltpu.SemaphoreType.DMA((grad_copies,)),
            pltpu.SemaphoreType.DMA((grad_copies,)),
        ],
        compiler_params=pltpu.CompilerParams(
            collective_id=1, has_side_effects=True, vmem_limit_bytes=VMEM_CAP
        ),
        name="step",
    )(data_points, noise_points, times.T, time_shift.reshape(1, hid_width), weight_in, weight_out)
    return pl.pallas_call(
        store_kernel,
        out_shape=(
            jax.ShapeDtypeStruct((share * steps_each, width), bf16),
            jax.ShapeDtypeStruct((width, hid_width), f32),
            jax.ShapeDtypeStruct((hid_width, width), f32),
        ),
        in_specs=[near, near],
        out_specs=(far, far, far),
        scratch_shapes=[pltpu.SemaphoreType.DMA((2 + hid_width // width,))],
        compiler_params=pltpu.CompilerParams(vmem_limit_bytes=1024 * 1024),
        name="store",
    )(*(pltpu.with_memory_space_constraint(a, pltpu.VMEM) for a in (predicted, summed)))


def solution(mesh):
    in_specs = (P("row", None), P("col", None), P(("row", "col"), None), P(), P(), P())
    out_specs = (P(("row", "col"), None), P(), P())
    return jax.shard_map(
        on_device, mesh=mesh, in_specs=in_specs, out_specs=out_specs, check_vma=False
    )
```
